32 devices in a mesh: dom: 8 (over z, x), feat: 4 (over y, core).
Axes of the slice: x: 2, y: 2, z: 4, core: 2. Of those that a mesh axis runs over, the one named last changes fastest.
Arguments:
- items: bfloat16 [2048, 1024], P('dom', 'feat'), may hold values from -6 to 6
- self_ids: int32 [2048], P('dom'), may hold values from 0 to 2047
- neighbor_ids: int32 [2048, 50], P('dom'), may hold values from 0 to 2047
- visit_counts: int32 [2048, 50], P('dom'), may hold values from 1 to 63
- w_self: bfloat16 [1024, 1024], P('feat'), may hold values from -0.1875 to 0.1875
- w_neighbor: bfloat16 [1024, 1024], P('feat'), may hold values from -0.75 to 0.75
- bias: float32 [1024], replicated, may hold values from -3 to 3
Outputs:
- embedding: float32 [2048, 1024], P('dom', 'feat')
The draws below stay inside these ranges and needn't reach their ends.
All inputs are finite; a program needn't handle non-finite values.
Results may differ from the reference program's by a relative error of at most 0.0018.
Values may be sent and summed in bfloat16 or wider, within the bound.
A program may use at most 64 MiB of HBM per device.

```python
import jax
import jax.numpy as jnp
from jax import lax

F = 1024
OUT = 1024
NBR = 50
ITEMS = 2048
BATCH = 2048


def set_ends(values, stream_key, low, high):
    longest = values.shape.index(max(values.shape))
    spots = []
    for shift in (0, 1):
        where = [jax.random.randint(jax.random.fold_in(stream_key, axis), (), 0, length) for axis, length in enumerate(values.shape)]
        where[longest] = (where[longest] + shift) % values.shape[longest]
        spots.append(tuple(where))
    return values.at[spots[0]].set(low).at[spots[1]].set(high)


def block_levels(own_key, dims, pieces, smallest, largest):
    factor_of, own = 1.0, jax.random.fold_in(own_key, 6)
    for axis_at, shards_of in pieces:
        steps = jnp.exp(jax.random.uniform(jax.random.fold_in(own, axis_at), (shards_of,), jnp.float32, smallest / len(pieces), largest / len(pieces)))
        factor_of = factor_of * jnp.repeat(steps, dims[axis_at] // shards_of).reshape([-1 if axis == axis_at else 1 for axis in range(len(dims))])
    return factor_of


def bell_draw(stream_key, dims, width, limit, pieces=(), held_as=jnp.bfloat16):
    drawn = width * jax.random.normal(stream_key, dims, jnp.float32)
    if pieces:
        drawn = drawn * block_levels(stream_key, dims, pieces, -0.22, 0.18)
    return jnp.clip(drawn, -limit, limit).astype(held_as)


def setup_inputs(seed: int = 0) -> dict:
    key_of = jax.random.split(jax.random.key(seed), 8)
    return {
        "items": bell_draw(key_of[0], (ITEMS, F), 1.0, 6.0, ((0, 8), (1, 4))),
        "self_ids": set_ends(jax.random.randint(key_of[1], (BATCH,), 0, ITEMS), jax.random.fold_in(key_of[1], 1), 0, ITEMS - 1).astype(jnp.int32),
        "neighbor_ids": set_ends(jax.random.randint(key_of[2], (BATCH, NBR), 0, ITEMS), jax.random.fold_in(key_of[2], 1), 0, ITEMS - 1).astype(jnp.int32),
        "visit_counts": set_ends(jax.random.randint(key_of[3], (BATCH, NBR), 1, 64), jax.random.fold_in(key_of[3], 1), 1, 63).astype(jnp.int32),
        "w_self": bell_draw(key_of[4], (F, OUT), F ** -0.5, 0.1875, ((0, 4),)),
        "w_neighbor": bell_draw(key_of[5], (F, OUT), (F // 16) ** -0.5, 0.75, ((0, 4),)),
        "bias": bell_draw(key_of[6], (OUT,), 0.5, 3.0, (), jnp.float32),
    }


def reference(items, self_ids, neighbor_ids, visit_counts, w_self, w_neighbor, bias):
    own = items[self_ids]
    total = lax.optimization_barrier(jnp.sum(visit_counts.astype(jnp.float32), axis=1))
    block = 512 if BATCH % 512 == 0 else BATCH
    ids_blocks = neighbor_ids.reshape(BATCH // block, block, NBR)
    count_blocks = visit_counts.reshape(BATCH // block, block, NBR)

    def pool(pair):
        ids, counts = pair
        rows = items[ids].astype(jnp.float32)
        return jnp.einsum('bk,bkf->bf', counts.astype(jnp.float32), rows)
    sums = lax.map(pool, (ids_blocks, count_blocks)).reshape(BATCH, F)
    pooled = (sums / total[:, None]).astype(jnp.bfloat16)
    pre = jnp.dot(own, w_self, preferred_element_type=jnp.float32) + jnp.dot(pooled, w_neighbor, preferred_element_type=jnp.float32)
    hidden = jnp.maximum(pre + bias[None, :], 0.0)
    scale = jnp.sqrt(lax.optimization_barrier(jnp.mean(hidden * hidden, axis=1, keepdims=True)) + 1e-06)
    return hidden / scale
```

```python
import functools

import jax
import jax.numpy as jnp
from jax import lax
from jax.experimental import pallas as pl
from jax.experimental.pallas import tpu as pltpu
from jax.sharding import PartitionSpec as P

MESH = pl.DeviceIdType.MESH
LANES = 128
GROUP = 8
PARTS = 4
SIDE = 2
CHUNKS = 2
PIECES = 2


def kernel(
    D, F,
    items_hbm, self_hbm, ids_hbm, cnt_hbm, ws_hbm, wn_hbm, bias_hbm,
    out_ref,
    selfs, ids_t, cnt_t, w_all, bias,
    ids, cnt, key_s, lo_s, wgt_s, weights, gathered, acc, both,
    send_a, recv_a, send_b, recv_b, sq_out, sq_in,
    local_sem,
    up_send, down_send, line_recv, x_send, x_recv,
    a_send_sem, a_recv_sem, b_send_sem, b_recv_sem, q_send_sem, q_recv_sem,
    side_send, side_recv, ready_up, ready_x, ready_feat,
):
    dom, feat = lax.axis_index("dom"), lax.axis_index("feat")
    Z, H = D // 2, F // 2
    z, x = dom // 2, lax.rem(dom, 2)
    y, c = feat // 2, lax.rem(feat, 2)
    R, FC = items_hbm.shape
    nb = selfs.shape[1]
    nbr = ids.shape[1]
    share = out_ref.shape[1]
    slot = key_s.shape[1] // GROUP
    n_hi = D * R // LANES
    part = R // PARTS
    other = dom + 1 - 2 * x

    barrier = pltpu.get_barrier_semaphore()
    line = [k for k in (1, 2) if k < Z]
    toward = 1 - 2 * lax.rem(z, 2)

    def signal(sem, d, f):
        pl.semaphore_signal(sem, inc=1, device_id=(d, f), device_id_type=MESH)

    for k in line:
        pl.when(z + k < Z)(functools.partial(signal, barrier, dom + 2 * k, feat))
    pl.when(x == 0)(functools.partial(signal, barrier, other, feat))
    for k in range(1, F):
        pl.when(feat + k < F)(functools.partial(signal, barrier, dom, feat + k))

    mine = pl.ds(pl.multiple_of(dom * R, R), R)
    pairs = (
        (ids_hbm, ids_t), (cnt_hbm, cnt_t), (self_hbm, selfs), (items_hbm, gathered.at[mine, :]),
        (ws_hbm, w_all.at[0:FC]), (wn_hbm, w_all.at[FC:2 * FC]),
    )
    local = [pltpu.make_async_copy(a, b, local_sem.at[min(i, 4)]) for i, (a, b) in enumerate(pairs)]
    for copy in local[0:3]:
        copy.start()
    lower = x + feat
    for k in line:
        lower = lower + (z >= k).astype(jnp.int32)
    pl.when(lower > 0)(lambda: pl.semaphore_wait(barrier, lower))

    def rows_of(block, h, n=1):
        return pl.ds(pl.multiple_of(block * R + h * part, part), n * part)

    def block_copy(block, h, n, own, send_sem, recv_sem, target):
        dst = gathered.at[rows_of(block, h, n), :]
        src = items_hbm.at[rows_of(0, h, n), :] if own else dst
        return pltpu.make_async_remote_copy(
            src_ref=src, dst_ref=dst, send_sem=send_sem, recv_sem=recv_sem,
            device_id=(target, feat), device_id_type=MESH,
        )

    def line_copy(s, h, sign, send, n=1):
        own = s < 2
        block = dom if own else dom - 2 * sign * s
        target = dom + 2 * sign * (s + 1 if own else 1)
        return block_copy(block, h, n, own, send.at[s], line_recv.at[(block // 2) * PARTS + h], target)

    def up_copy(s, h, n=1):
        return line_copy(s, h, 1, up_send, n)

    def down_copy(s, h, n=1):
        return line_copy(s, h, -1, down_send, n)

    def line_arrived(step, h):
        block = dom + 2 * step
        block_copy(block, h, 1, False, up_send.at[0], line_recv.at[(block // 2) * PARTS + h], dom).wait_recv()

    def x_copy(step, h, n=1):
        own = isinstance(step, int) and step == 0
        return block_copy(dom + 2 * step, h, n, own, x_send.at[z + step], x_recv.at[z + step], other)

    def x_arrived(step, n=PARTS):
        block_copy(other + 2 * step, 0, n, False, x_send.at[z + step], x_recv.at[z + step], dom).wait_recv()

    def side_copy(h, n=1):
        return block_copy(other, h, n, False, side_send, side_recv, dom + 2 * toward)

    inner = (z > 0) & (z < Z - 1)

    def own_down(s):
        for h in range(PARTS):
            down_copy(s, h).start()

    for k in reversed(line):
        pl.when(inner & (z >= k))(functools.partial(own_down, k - 1))
    for k in line:
        pl.when(z == Z - 1)(functools.partial(own_down, k - 1))

    def across():
        for h in range(PARTS):
            x_copy(0, h).start()

    pl.when(x == 1)(across)
    for k in line:
        pl.when(z >= k)(functools.partial(signal, ready_up.at[k - 1], dom - 2 * k, feat))
    pl.when(x == 1)(functools.partial(signal, ready_x, other, feat))
    for k in range(1, F):
        pl.when(feat >= k)(functools.partial(signal, ready_feat, dom, feat - k))
    for copy in local[3:]:
        copy.start()
    bias_load = pltpu.make_async_copy(bias_hbm, bias, local_sem.at[5])
    bias_load.start()

    def over_x(s, h, sign):
        if s > 0:
            x_copy(sign * (s + 1), h).start()
        else:
            @pl.when((h < SIDE) | (toward != sign))
            def _():
                x_copy(sign, h).start()

    def from_above(s, h):
        @pl.when(z < Z - 1 - s)
        def _():
            line_arrived(s + 1, h)
            if 0 < s < Z - 2:
                pl.when(z > 0)(lambda: down_copy(s + 1, h).start())
            over_x(s, h, 1)

    def from_below(s, h):
        @pl.when(z > s)
        def _():
            line_arrived(-(s + 1), h)
            if 0 < s < Z - 2:
                pl.when(z < Z - 1)(lambda: up_copy(s + 1, h).start())
            over_x(s, h, -1)

    def forward(s, h):
        pl.when(z < Z // 2)(lambda: from_below(s, h))
        from_above(s, h)
        pl.when(z >= Z // 2)(lambda: from_below(s, h))

    def sides():
        x_arrived(0)
        for h in range(SIDE, PARTS):
            side_copy(h).start()

    for copy in local[0:3]:
        copy.wait()
    ids[...] = jnp.transpose(ids_t[...])
    cnt[...] = jnp.transpose(cnt_t[...])
    wgt_s[...] = jnp.zeros_like(wgt_s)
    lo_s[...] = jnp.zeros_like(lo_s)
    key_s[...] = jnp.zeros_like(key_s)
    for j in range(GROUP):
        ids_j = ids[pl.ds(j, nb // GROUP, stride=GROUP), :]
        at = slice(j * slot, j * slot + nbr)
        key_s[:, at] = (ids_j // LANES) * GROUP + j
        lo_s[:, at] = lax.rem(ids_j, LANES)
        wgt_s[:, at] = cnt[pl.ds(j, nb // GROUP, stride=GROUP), :].astype(jnp.float32)

    K = key_s.shape[1]

    def half_group(g):
        key = key_s[pl.ds(g, 1), :]
        low = lo_s[pl.ds(g, 1), :]
        wgt = wgt_s[pl.ds(g, 1), :]
        left = jnp.where(lax.broadcasted_iota(jnp.int32, (n_hi * GROUP, K), 0) == key, wgt, 0.0)
        right = jnp.where(lax.broadcasted_iota(jnp.int32, (LANES, K), 0) == low, 1.0, 0.0)
        return lax.dot_general(
            left.astype(jnp.bfloat16), right.astype(jnp.bfloat16),
            (((1,), (1,)), ((), ())), preferred_element_type=jnp.float32,
        )

    def build(it, carry):
        first, second = half_group(it * 2), half_group(it * 2 + 1)
        at = pl.ds(pl.multiple_of(nb + it * 2 * GROUP, 2 * GROUP), 2 * GROUP)
        for hi in range(n_hi):
            rows = slice(hi * GROUP, (hi + 1) * GROUP)
            tile = jnp.concatenate([first[rows], second[rows]], axis=0)
            weights[at, hi * LANES:(hi + 1) * LANES] = tile.astype(jnp.bfloat16)
        return carry

    def build_pair(it, carry):
        return build(it * 2 + 1, build(it * 2, carry))

    self_col = jnp.transpose(jnp.broadcast_to(selfs[...], (LANES, nb)))
    lane = lax.broadcasted_iota(jnp.int32, (nb, LANES), 1)
    inverse = 1.0 / jnp.sum(cnt[...].astype(jnp.float32), axis=1, keepdims=True)

    @pl.when(x == 0)
    def _():
        pl.semaphore_wait(ready_x, 1)
        across()

    def own_up(k):
        pl.semaphore_wait(ready_up.at[k - 1], 1)
        for h in range(PARTS):
            up_copy(k - 1, h).start()

    for k in reversed(line):
        pl.when(inner & (z + k < Z))(functools.partial(own_up, k))
    for k in line:
        pl.when(z == 0)(functools.partial(own_up, k))

    units = nb // (4 * GROUP)
    early = units - PARTS * (-(-units // (2 * PARTS)))
    late = units - early
    lax.fori_loop(0, early, build_pair, 0)
    for h in range(SIDE):
        pl.when(z == 0)(functools.partial(from_above, 0, h))
        pl.when(z == Z - 1)(functools.partial(from_below, 0, h))

    def slot(h, carry):
        carry = lax.fori_loop(early + late * h // PARTS, early + late * (h + 1) // PARTS, build_pair, carry)
        forward(1, h)
        return carry

    lax.fori_loop(0, PARTS, slot, 0)
    sides()

    def self_weights():
        for hi in range(n_hi):
            hit = jnp.where(self_col == lane + hi * LANES, 1.0, 0.0)
            weights[0:nb, hi * LANES:(hi + 1) * LANES] = hit.astype(jnp.bfloat16)

    def add(block, low, high):
        rows = pl.ds(pl.multiple_of(block * R + low * part, part), (high - low) * part)
        at = pl.ds(pl.multiple_of(block * R + low * part, LANES), (high - low) * part)
        acc[...] += jnp.dot(weights[:, at], gathered[rows, :], preferred_element_type=jnp.float32)

    def if_there(step, work):
        pl.when((z + step >= 0) & (z + step < Z))(work)

    def add_z(step):
        def work():
            add(dom + 2 * step, 0, PARTS)
        if_there(step, work)

    def add_x(step):
        def work():
            x_arrived(step)
            add(other + 2 * step, 0, PARTS)
        if_there(step, work)

    def add_pair():
        x_arrived(toward, SIDE)
        block_copy(other + 2 * toward, SIDE, PARTS - SIDE, False, side_send, side_recv, dom).wait_recv()
        add(other + 2 * toward, 0, PARTS)

    def add_next():
        def work():
            x_arrived(-toward)
            add(other - 2 * toward, 0, PARTS)
        pl.when((z - toward >= 0) & (z - toward < Z))(work)

    def both_ways(work, s):
        work(-s)
        work(s)

    def first_dots():
        local[3].wait()
        acc[...] = jnp.dot(weights[:, mine], gathered[mine, :], preferred_element_type=jnp.float32)
        add(other, 0, PARTS)

    todo = [self_weights, first_dots, functools.partial(both_ways, add_z, 2)]
    for h in range(PARTS):
        if h < len(todo):
            todo[h]()
        if h < SIDE:
            pl.when(inner)(functools.partial(forward, 0, h))
        else:
            forward(0, h)
    for s in range(2, Z - 1):
        todo = [functools.partial(both_ways, add_z, 1)] if s == 2 else [functools.partial(both_ways, add_z, s)]
        for h in range(PARTS):
            if h < len(todo):
                todo[h]()
            forward(s, h)
    both_ways(add_z, Z - 1)
    both_ways(add_x, 2)
    add_pair()
    add_next()
    for s in range(3, Z):
        both_ways(add_x, s)

    pltpu.make_async_copy(w_all, w_all, local_sem.at[4]).wait()
    bias_load.wait()
    pl.when(feat < F - 1)(lambda: pl.semaphore_wait(ready_feat, F - 1 - feat))
    both[:, 0:FC] = acc[0:nb, :].astype(jnp.bfloat16)
    both[:, FC:2 * FC] = (acc[nb:2 * nb, :] * inverse).astype(jnp.bfloat16)
    tall = nb // CHUNKS
    short = tall // PIECES

    def chunk(r):
        return pl.ds(r * tall, tall)

    def project(r, yy, cc):
        cols = pl.ds(pl.multiple_of((yy * 2 + cc) * share, share), share)
        return jnp.dot(both[chunk(r), :], w_all[:, cols], preferred_element_type=jnp.float32)

    def a_copy(k, r):
        i = k * CHUNKS + r
        return pltpu.make_async_remote_copy(
            src_ref=send_a.at[k, chunk(r)], dst_ref=recv_a.at[k, chunk(r)],
            send_sem=a_send_sem, recv_sem=a_recv_sem.at[i],
            device_id=(dom, feat + 1 - 2 * c), device_id_type=MESH,
        )

    def b_copy(k, p):
        i = k * CHUNKS * PIECES + p
        at = pl.ds(p * short, short)
        return pltpu.make_async_remote_copy(
            src_ref=send_b.at[k, at], dst_ref=recv_b.at[k, at], send_sem=b_send_sem, recv_sem=b_recv_sem.at[i],
            device_id=(dom, lax.rem(y + k + 1, H) * 2 + c), device_id_type=MESH,
        )

    def q_copy(k, r):
        return pltpu.make_async_remote_copy(
            src_ref=sq_out.at[r], dst_ref=sq_in.at[r, k - 1], send_sem=q_send_sem, recv_sem=q_recv_sem.at[r],
            device_id=(dom, lax.rem(feat + k, F)), device_id_type=MESH,
        )

    def all_of(ref, send_sem, recv_sem):
        return pltpu.make_async_remote_copy(
            src_ref=ref, dst_ref=ref, send_sem=send_sem, recv_sem=recv_sem, device_id=(dom, feat), device_id_type=MESH,
        )

    for k in range(H):
        yy = lax.rem(y + k + 1, H)
        for r in range(CHUNKS):
            send_a[k, chunk(r)] = project(r, yy, 1 - c)
            a_copy(k, r).start()
        for r in range(CHUNKS):
            here = project(r, yy, c)
            a_copy(k, r).wait_recv()
            summed = here + recv_a[k, chunk(r)]
            if k < H - 1:
                send_b[k, chunk(r)] = summed.astype(jnp.bfloat16)
                for p in range(r * PIECES, (r + 1) * PIECES):
                    b_copy(k, p).start()
            else:
                out_ref[chunk(r), :] = summed + bias[:, pl.ds(pl.multiple_of(feat * share, share), share)]

    for s in range(Z - 1):
        pl.when((z + s + 1 < Z) if s < 2 else (z < Z - 1) & (z >= s))(lambda: up_copy(s, 0, PARTS).wait_send())
        pl.when((z > s) if s < 2 else (z > 0) & (z + s < Z))(lambda: down_copy(s, 0, PARTS).wait_send())
    side_copy(SIDE, PARTS - SIDE).wait_send()
    x_copy(0, 0, PARTS).wait_send()
    x_copy(toward, 0, SIDE).wait_send()
    pl.when((z - toward >= 0) & (z - toward < Z))(lambda: x_copy(-toward, 0, PARTS).wait_send())
    for step in range(2, Z):
        pl.when(z + step < Z)(lambda: x_copy(step, 0, PARTS).wait_send())
        pl.when(z >= step)(lambda: x_copy(-step, 0, PARTS).wait_send())

    for r in range(CHUNKS):
        squares = []
        for p in range(r * PIECES, (r + 1) * PIECES):
            at = pl.ds(p * short, short)
            total = out_ref[at, :]
            for k in range(H - 1):
                b_copy(k, p).wait_recv()
                total = total + recv_b[k, at].astype(jnp.float32)
            hidden = jnp.maximum(total, 0.0)
            out_ref[at, :] = hidden
            square = hidden * hidden
            folded = square[:, 0:LANES]
            for i in range(1, share // LANES):
                folded = folded + square[:, i * LANES:(i + 1) * LANES]
            squares.append(folded)
        turned = jnp.transpose(jnp.concatenate(squares, axis=0))
        row = jnp.sum(turned, axis=0, keepdims=True)
        sq_out[r] = jnp.broadcast_to(row, (GROUP, tall))
        for k in range(1, F):
            q_copy(k, r).start()

    for r in range(CHUNKS):
        all_of(sq_in.at[r], q_send_sem, q_recv_sem.at[r]).wait_recv()
        row = sq_out[r]
        for k in range(1, F):
            row = row + sq_in[r, k - 1]
        scale = lax.rsqrt(row / (share * F) + 1e-06)[0:1, :]
        column = jnp.transpose(jnp.broadcast_to(scale, (LANES, tall)))
        for i in range(share // LANES):
            at = slice(i * LANES, (i + 1) * LANES)
            out_ref[chunk(r), at] = out_ref[chunk(r), at] * column

    all_of(send_a, a_send_sem, a_recv_sem.at[0]).wait_send()
    all_of(send_b, b_send_sem, b_recv_sem.at[0]).wait_send()
    all_of(sq_in, q_send_sem, q_recv_sem.at[0]).wait_send()


def shards(D, F, items, self_ids, neighbor_ids, visit_counts, w_self, w_neighbor, bias):
    R, FC = items.shape
    nb, nbr = neighbor_ids.shape
    out = bias.shape[0]
    share = out // F
    slot = 1 << (nbr - 1).bit_length()
    Z, H = D // 2, F // 2
    f32, bf16, i32 = jnp.float32, jnp.bfloat16, jnp.int32
    dma, flag = pltpu.SemaphoreType.DMA, pltpu.SemaphoreType.REGULAR
    return pl.pallas_call(
        functools.partial(kernel, D, F),
        out_shape=pltpu.VMEM((nb, share), f32),
        in_specs=[pl.BlockSpec(memory_space=pl.ANY)] * 7,
        out_specs=pl.BlockSpec(memory_space=pltpu.VMEM),
        scratch_shapes=[
            pltpu.VMEM((1, nb), i32),
            pltpu.VMEM((nbr, nb), i32),
            pltpu.VMEM((nbr, nb), i32),
            pltpu.VMEM((2 * FC, out), bf16),
            pltpu.VMEM((1, out), f32),
            pltpu.VMEM((nb, nbr), i32),
            pltpu.VMEM((nb, nbr), i32),
            pltpu.VMEM((nb // GROUP, GROUP * slot), i32),
            pltpu.VMEM((nb // GROUP, GROUP * slot), i32),
            pltpu.VMEM((nb // GROUP, GROUP * slot), f32),
            pltpu.VMEM((2 * nb, D * R), bf16),
            pltpu.VMEM((D * R, FC), bf16),
            pltpu.VMEM((2 * nb, FC), f32),
            pltpu.VMEM((nb, 2 * FC), bf16),
            pltpu.VMEM((H, nb, share), f32),
            pltpu.VMEM((H, nb, share), f32),
            pltpu.VMEM((H - 1, nb, share), bf16),
            pltpu.VMEM((H - 1, nb, share), bf16),
            pltpu.VMEM((CHUNKS, GROUP, nb // CHUNKS), f32),
            pltpu.VMEM((CHUNKS, F - 1, GROUP, nb // CHUNKS), f32),
            dma((6,)),
            dma((Z - 1,)), dma((Z - 1,)), dma((Z * PARTS,)), dma((Z,)), dma((Z,)),
            dma, dma((H * CHUNKS,)), dma, dma(((H - 1) * CHUNKS * PIECES,)), dma, dma((CHUNKS,)),
            dma, dma, flag((2,)), flag, flag,
        ],
        compiler_params=pltpu.CompilerParams(collective_id=0, has_side_effects=True),
    )(items, self_ids.reshape(1, nb), neighbor_ids.T, visit_counts.T, w_self, w_neighbor, bias.reshape(1, out))


def solution(mesh):
    placed = (
        P("dom", "feat"),
        P("dom"),
        P("dom", None),
        P("dom", None),
        P("feat", None),
        P("feat", None),
        P(),
    )
    return jax.shard_map(
        functools.partial(shards, mesh.shape["dom"], mesh.shape["feat"]),
        mesh=mesh, in_specs=placed, out_specs=P("dom", "feat"), check_vma=False,
    )
```

```python
import functools

import jax
import jax.numpy as jnp
from jax import lax
from jax.experimental import pallas as pl
from jax.experimental.pallas import tpu as pltpu
from jax.sharding import PartitionSpec as P

MESH = pl.DeviceIdType.MESH
LANES = 128
GROUP = 8
PARTS = 4
SIDE = 2
CHUNKS = 2
PIECES = 2


def kernel(
    D, F,
    items_hbm, self_hbm, ids_hbm, cnt_hbm, ws_hbm, wn_hbm, bias_hbm,
    out_ref,
    selfs, ids_t, cnt_t, w_all, bias,
    ids, cnt, key_s, lo_s, wgt_s, weights, gathered, acc, both,
    send_a, recv_a, send_b, recv_b, sq_out, sq_in,
    local_sem,
    up_send, down_send, line_recv, x_send, x_recv,
    a_send_sem, a_recv_sem, b_send_sem, b_recv_sem, q_send_sem, q_recv_sem,
    side_send, side_recv, ready_up, ready_x, ready_feat,
):
    dom, feat = lax.axis_index("dom"), lax.axis_index("feat")
    Z, H = D // 2, F // 2
    z, x = dom // 2, lax.rem(dom, 2)
    y, c = feat // 2, lax.rem(feat, 2)
    R, FC = items_hbm.shape
    nb = selfs.shape[1]
    nbr = ids.shape[1]
    share = out_ref.shape[1]
    slot = key_s.shape[1] // GROUP
    n_hi = D * R // LANES
    part = R // PARTS
    other = dom + 1 - 2 * x

    barrier = pltpu.get_barrier_semaphore()
    line = [k for k in (1, 2) if k < Z]
    lower, upper = z < Z // 2, z >= Z // 2
    inward = jnp.where(lower, 1, -1)

    def signal(sem, d, f):
        pl.semaphore_signal(sem, inc=1, device_id=(d, f), device_id_type=MESH)

    for k in line:
        pl.when(z + k < Z)(functools.partial(signal, barrier, dom + 2 * k, feat))
    pl.when(x == 0)(functools.partial(signal, barrier, other, feat))
    for k in range(1, F):
        pl.when(feat + k < F)(functools.partial(signal, barrier, dom, feat + k))

    mine = pl.ds(pl.multiple_of(dom * R, R), R)
    pairs = (
        (ids_hbm, ids_t), (cnt_hbm, cnt_t), (self_hbm, selfs), (items_hbm, gathered.at[mine, :]),
        (ws_hbm, w_all.at[0:FC]), (wn_hbm, w_all.at[FC:2 * FC]),
    )
    local = [pltpu.make_async_copy(a, b, local_sem.at[min(i, 4)]) for i, (a, b) in enumerate(pairs)]
    for copy in local[0:3]:
        copy.start()
    below = x + feat
    for k in line:
        below = below + (z >= k).astype(jnp.int32)
    pl.when(below > 0)(lambda: pl.semaphore_wait(barrier, below))

    def rows_of(block, h, n=1):
        return pl.ds(pl.multiple_of(block * R + h * part, part), n * part)

    def block_copy(block, h, n, own, send_sem, recv_sem, target):
        dst = gathered.at[rows_of(block, h, n), :]
        src = items_hbm.at[rows_of(0, h, n), :] if own else dst
        return pltpu.make_async_remote_copy(
            src_ref=src, dst_ref=dst, send_sem=send_sem, recv_sem=recv_sem,
            device_id=(target, feat), device_id_type=MESH,
        )

    def line_copy(s, h, sign, send, n=1):
        own = s < 2
        block = dom if own else dom - 2 * sign * s
        target = dom + 2 * sign * (s + 1 if own else 1)
        return block_copy(block, h, n, own, send.at[s], line_recv.at[(block // 2) * PARTS + h], target)

    def up_copy(s, h, n=1):
        return line_copy(s, h, 1, up_send, n)

    def down_copy(s, h, n=1):
        return line_copy(s, h, -1, down_send, n)

    def line_arrived(step, h):
        block = dom + 2 * step
        block_copy(block, h, 1, False, up_send.at[0], line_recv.at[(block // 2) * PARTS + h], dom).wait_recv()

    def x_copy(step, h, n=1):
        at = Z if step == 0 and h >= SIDE else z + step
        return block_copy(dom + 2 * step, h, n, step == 0, x_send.at[z + step], x_recv.at[at], other)

    def x_arrived(step, h, n):
        at = Z if h >= SIDE else z + step
        block_copy(other + 2 * step, h, n, False, x_send.at[z + step], x_recv.at[at], dom).wait_recv()

    def side_down(target):
        return block_copy(D - 1 - x, SIDE, PARTS - SIDE, False, side_send.at[0], side_recv.at[0], target)

    def side_up(target):
        return block_copy(1 - x, SIDE, PARTS - SIDE, False, side_send.at[1], side_recv.at[1], target)

    inner, outer = (z > 0) & (z < Z - 1), (z == 0) | (z == Z - 1)

    def own_down(s):
        for h in range(PARTS):
            down_copy(s, h).start()

    for k in reversed(line):
        pl.when(inner & (z >= k))(functools.partial(own_down, k - 1))
    pl.when(z == Z - 1)(functools.partial(own_down, line[-1] - 1))

    def across():
        for h in [*range(SIDE, PARTS), *range(SIDE)]:
            x_copy(0, h).start()

    pl.when(x == 1)(across)
    for k in line:
        pl.when(z >= k)(functools.partial(signal, ready_up.at[k - 1], dom - 2 * k, feat))
    pl.when(x == 1)(functools.partial(signal, ready_x, other, feat))
    for k in range(1, F):
        pl.when(feat >= k)(functools.partial(signal, ready_feat, dom, feat - k))
    for copy in local[3:]:
        copy.start()
    bias_load = pltpu.make_async_copy(bias_hbm, bias, local_sem.at[5])
    bias_load.start()

    def over_x(s, h, sign):
        if s == 0:
            x_copy(sign, h).start()
        else:
            end = z + s + 1 == Z - 1 if sign > 0 else z - s - 1 == 0

            @pl.when((h < SIDE) | jnp.logical_not(end))
            def _():
                x_copy(sign * (s + 1), h).start()

    def from_above(s, h):
        @pl.when(z < Z - 1 - s)
        def _():
            line_arrived(s + 1, h)
            if 0 < s < Z - 2:
                pl.when(z > 0)(lambda: down_copy(s + 1, h).start())
            over_x(s, h, 1)

    def from_below(s, h):
        @pl.when(z > s)
        def _():
            line_arrived(-(s + 1), h)
            if 0 < s < Z - 2:
                pl.when(z < Z - 1)(lambda: up_copy(s + 1, h).start())
            over_x(s, h, -1)

    def forward(s, h):
        from_above(s, h)
        from_below(s, h)

    def pass_sides():
        @pl.when((z > 0) & (z < Z - 2))
        def _():
            side_down(dom).wait_recv()
            side_down(dom - 2).start()

        @pl.when((z > 1) & (z < Z - 1))
        def _():
            side_up(dom).wait_recv()
            side_up(dom + 2).start()

    for copy in local[0:3]:
        copy.wait()
    ids[...] = jnp.transpose(ids_t[...])
    cnt[...] = jnp.transpose(cnt_t[...])
    wgt_s[...] = jnp.zeros_like(wgt_s)
    lo_s[...] = jnp.zeros_like(lo_s)
    key_s[...] = jnp.zeros_like(key_s)
    for j in range(GROUP):
        ids_j = ids[pl.ds(j, nb // GROUP, stride=GROUP), :]
        at = slice(j * slot, j * slot + nbr)
        key_s[:, at] = (ids_j // LANES) * GROUP + j
        lo_s[:, at] = lax.rem(ids_j, LANES)
        wgt_s[:, at] = cnt[pl.ds(j, nb // GROUP, stride=GROUP), :].astype(jnp.float32)

    K = key_s.shape[1]

    def half_group(g):
        key = key_s[pl.ds(g, 1), :]
        low = lo_s[pl.ds(g, 1), :]
        wgt = wgt_s[pl.ds(g, 1), :]
        left = jnp.where(lax.broadcasted_iota(jnp.int32, (n_hi * GROUP, K), 0) == key, wgt, 0.0)
        right = jnp.where(lax.broadcasted_iota(jnp.int32, (LANES, K), 0) == low, 1.0, 0.0)
        return lax.dot_general(
            left.astype(jnp.bfloat16), right.astype(jnp.bfloat16),
            (((1,), (1,)), ((), ())), preferred_element_type=jnp.float32,
        )

    def build(it, carry):
        first, second = half_group(it * 2), half_group(it * 2 + 1)
        at = pl.ds(pl.multiple_of(nb + it * 2 * GROUP, 2 * GROUP), 2 * GROUP)
        for hi in range(n_hi):
            rows = slice(hi * GROUP, (hi + 1) * GROUP)
            tile = jnp.concatenate([first[rows], second[rows]], axis=0)
            weights[at, hi * LANES:(hi + 1) * LANES] = tile.astype(jnp.bfloat16)
        return carry

    def build_pair(it, carry):
        return build(it * 2 + 1, build(it * 2, carry))

    self_col = jnp.transpose(jnp.broadcast_to(selfs[...], (LANES, nb)))
    lane = lax.broadcasted_iota(jnp.int32, (nb, LANES), 1)
    inverse = 1.0 / jnp.sum(cnt[...].astype(jnp.float32), axis=1, keepdims=True)

    @pl.when(x == 0)
    def _():
        pl.semaphore_wait(ready_x, 1)
        across()

    def own_up(k):
        pl.semaphore_wait(ready_up.at[k - 1], 1)
        for h in range(PARTS):
            up_copy(k - 1, h).start()

    for k in line:
        pl.when(z + k < Z)(functools.partial(own_up, k))

    units = nb // (4 * GROUP)
    early = units - PARTS * (-(-units // (2 * PARTS)))
    late = units - early
    lax.fori_loop(0, early, build_pair, 0)
    x_arrived(0, SIDE, PARTS - SIDE)
    pl.when(z == 0)(lambda: side_up(dom + 4).start())

    @pl.when(z == Z - 1)
    def _():
        side_down(dom - 4).start()
        own_down(0)

    def slot(h, carry):
        carry = lax.fori_loop(early + late * h // PARTS, early + late * (h + 1) // PARTS, build_pair, carry)
        pl.when(inner & (lower | (h < SIDE)))(lambda: from_below(0, h))
        pl.when(inner)(lambda: forward(1, h))
        pl.when(outer)(lambda: forward(0, h))
        return carry

    lax.fori_loop(0, PARTS, slot, 0)

    def self_weights():
        for hi in range(n_hi):
            hit = jnp.where(self_col == lane + hi * LANES, 1.0, 0.0)
            weights[0:nb, hi * LANES:(hi + 1) * LANES] = hit.astype(jnp.bfloat16)

    def add(block, low, high):
        rows = pl.ds(pl.multiple_of(block * R + low * part, part), (high - low) * part)
        at = pl.ds(pl.multiple_of(block * R + low * part, LANES), (high - low) * part)
        acc[...] += jnp.dot(weights[:, at], gathered[rows, :], preferred_element_type=jnp.float32)

    def if_there(step, work):
        pl.when((z + step >= 0) & (z + step < Z))(work)

    def add_z(step):
        def work():
            add(dom + 2 * step, 0, PARTS)
        if_there(step, work)

    def add_x(step):
        def work():
            end = z + step == (Z - 1 if step > 0 else 0)
            pl.when(end)(lambda: x_arrived(step, 0, SIDE))
            pl.when(jnp.logical_not(end))(lambda: x_arrived(step, 0, PARTS))
            pl.when(end & (z == 0))(lambda: side_down(dom).wait_recv())
            pl.when(end & (z == Z - 1))(lambda: side_up(dom).wait_recv())
            add(other + 2 * step, 0, PARTS)
        if_there(step, work)

    def add_next(step):
        def work():
            x_arrived(step, 0, PARTS)
            add(other + 2 * step, 0, PARTS)
        if_there(step, work)

    def both_ways(work, s):
        work(-s)
        work(s)

    def first_dots():
        local[3].wait()
        acc[...] = jnp.dot(weights[:, mine], gathered[mine, :], preferred_element_type=jnp.float32)
        x_arrived(0, 0, SIDE)
        add(other, 0, PARTS)

    near, far = jnp.where(outer, 1, 2), jnp.where(outer, 2, 1)
    self_weights()
    first_dots()
    both_ways(add_z, near)
    pass_sides()
    first, final = z == 0, z == Z - 1
    for h in range(PARTS):
        pl.when(inner)(functools.partial(from_above, 0, h))
        if h >= SIDE:
            pl.when(inner & upper)(functools.partial(from_below, 0, h))
    for s, h in ((1, 0), (1, 1), (2, 0), (1, 2), (2, 1), (1, 3)):
        pl.when(first)(functools.partial(from_above, s, h))
    for s, h in ((1, 0), (1, 1), (2, 0), (1, 2), (2, 1), (1, 3)):
        pl.when(final)(functools.partial(from_below, s, h))
    for h in range(SIDE, PARTS):
        pl.when(outer)(functools.partial(forward, 2, h))
    for s in range(2, Z - 1):
        for h in range(PARTS):
            if s < Z - 2:
                pl.when(inner)(functools.partial(forward, s, h))
            if s > 2:
                pl.when(outer)(functools.partial(forward, s, h))
    for s in range(3, Z):
        both_ways(add_z, s)
    both_ways(add_z, far)
    add_next(jnp.where(outer, inward, -inward))
    pl.when(inner)(functools.partial(both_ways, add_x, 2))
    for s in range(3, Z):
        both_ways(add_x, s)
    add_next(jnp.where(outer, 2 * inward, inward))

    pltpu.make_async_copy(w_all, w_all, local_sem.at[4]).wait()
    bias_load.wait()
    pl.when(feat < F - 1)(lambda: pl.semaphore_wait(ready_feat, F - 1 - feat))
    tall = nb // CHUNKS
    short = tall // PIECES

    def chunk(r):
        return pl.ds(r * tall, tall)

    def combine(r):
        at = slice(r * tall, (r + 1) * tall)
        both[at, 0:FC] = acc[at, :].astype(jnp.bfloat16)
        both[at, FC:2 * FC] = (acc[nb + r * tall:nb + (r + 1) * tall, :] * inverse[at]).astype(jnp.bfloat16)

    def project(r, yy, cc):
        cols = pl.ds(pl.multiple_of((yy * 2 + cc) * share, share), share)
        return jnp.dot(both[chunk(r), :], w_all[:, cols], preferred_element_type=jnp.float32)

    def a_copy(k, r):
        i = k * CHUNKS + r
        return pltpu.make_async_remote_copy(
            src_ref=send_a.at[k, chunk(r)], dst_ref=recv_a.at[k, chunk(r)],
            send_sem=a_send_sem, recv_sem=a_recv_sem.at[i],
            device_id=(dom, feat + 1 - 2 * c), device_id_type=MESH,
        )

    def b_copy(k, p):
        i = k * CHUNKS * PIECES + p
        at = pl.ds(p * short, short)
        return pltpu.make_async_remote_copy(
            src_ref=send_b.at[k, at], dst_ref=recv_b.at[k, at], send_sem=b_send_sem, recv_sem=b_recv_sem.at[i],
            device_id=(dom, lax.rem(y + k + 1, H) * 2 + c), device_id_type=MESH,
        )

    def q_copy(k, r):
        return pltpu.make_async_remote_copy(
            src_ref=sq_out.at[r], dst_ref=sq_in.at[r, k - 1], send_sem=q_send_sem, recv_sem=q_recv_sem.at[r],
            device_id=(dom, lax.rem(feat + k, F)), device_id_type=MESH,
        )

    def all_of(ref, send_sem, recv_sem):
        return pltpu.make_async_remote_copy(
            src_ref=ref, dst_ref=ref, send_sem=send_sem, recv_sem=recv_sem, device_id=(dom, feat), device_id_type=MESH,
        )

    for k in range(H):
        yy = lax.rem(y + k + 1, H)
        for r in range(CHUNKS):
            if k == 0:
                combine(r)
            send_a[k, chunk(r)] = project(r, yy, 1 - c)
            a_copy(k, r).start()
        for r in range(CHUNKS):
            here = project(r, yy, c)
            a_copy(k, r).wait_recv()
            summed = here + recv_a[k, chunk(r)]
            if k < H - 1:
                send_b[k, chunk(r)] = summed.astype(jnp.bfloat16)
                for p in range(r * PIECES, (r + 1) * PIECES):
                    b_copy(k, p).start()
            else:
                out_ref[chunk(r), :] = summed + bias[:, pl.ds(pl.multiple_of(feat * share, share), share)]

    for s in range(Z - 1):
        pl.when((z + s + 1 < Z) if s < 2 else (z < Z - 1) & (z >= s))(lambda: up_copy(s, 0, PARTS).wait_send())
        pl.when((z > s) if s < 2 else (z > 0) & (z + s < Z))(lambda: down_copy(s, 0, PARTS).wait_send())
    pl.when((z == Z - 1) | (z > 0) & (z < Z - 2))(lambda: side_down(dom - 2).wait_send())
    pl.when((z == 0) | (z > 1) & (z < Z - 1))(lambda: side_up(dom + 2).wait_send())

    def x_sent(step):
        if abs(step) < 2:
            x_copy(step, 0, PARTS).wait_send()
        else:
            end = z + step == (Z - 1 if step > 0 else 0)
            pl.when(end)(lambda: x_copy(step, 0, SIDE).wait_send())
            pl.when(jnp.logical_not(end))(lambda: x_copy(step, 0, PARTS).wait_send())

    for step in range(-(Z - 1), Z):
        if_there(step, functools.partial(x_sent, step))

    for r in range(CHUNKS):
        squares = []
        for p in range(r * PIECES, (r + 1) * PIECES):
            at = pl.ds(p * short, short)
            total = out_ref[at, :]
            for k in range(H - 1):
                b_copy(k, p).wait_recv()
                total = total + recv_b[k, at].astype(jnp.float32)
            hidden = jnp.maximum(total, 0.0)
            out_ref[at, :] = hidden
            square = hidden * hidden
            folded = square[:, 0:LANES]
            for i in range(1, share // LANES):
                folded = folded + square[:, i * LANES:(i + 1) * LANES]
            squares.append(folded)
        turned = jnp.transpose(jnp.concatenate(squares, axis=0))
        row = jnp.sum(turned, axis=0, keepdims=True)
        sq_out[r] = jnp.broadcast_to(row, (GROUP, tall))
        for k in range(1, F):
            q_copy(k, r).start()

    for r in range(CHUNKS):
        all_of(sq_in.at[r], q_send_sem, q_recv_sem.at[r]).wait_recv()
        row = sq_out[r]
        for k in range(1, F):
            row = row + sq_in[r, k - 1]
        scale = lax.rsqrt(row / (share * F) + 1e-06)[0:1, :]
        column = jnp.transpose(jnp.broadcast_to(scale, (LANES, tall)))
        for i in range(share // LANES):
            at = slice(i * LANES, (i + 1) * LANES)
            out_ref[chunk(r), at] = out_ref[chunk(r), at] * column

    all_of(send_a, a_send_sem, a_recv_sem.at[0]).wait_send()
    all_of(send_b, b_send_sem, b_recv_sem.at[0]).wait_send()
    all_of(sq_in, q_send_sem, q_recv_sem.at[0]).wait_send()


def shards(D, F, items, self_ids, neighbor_ids, visit_counts, w_self, w_neighbor, bias):
    R, FC = items.shape
    nb, nbr = neighbor_ids.shape
    out = bias.shape[0]
    share = out // F
    slot = 1 << (nbr - 1).bit_length()
    Z, H = D // 2, F // 2
    f32, bf16, i32 = jnp.float32, jnp.bfloat16, jnp.int32
    dma, flag = pltpu.SemaphoreType.DMA, pltpu.SemaphoreType.REGULAR
    return pl.pallas_call(
        functools.partial(kernel, D, F),
        out_shape=pltpu.VMEM((nb, share), f32),
        in_specs=[pl.BlockSpec(memory_space=pl.ANY)] * 7,
        out_specs=pl.BlockSpec(memory_space=pltpu.VMEM),
        scratch_shapes=[
            pltpu.VMEM((1, nb), i32),
            pltpu.VMEM((nbr, nb), i32),
            pltpu.VMEM((nbr, nb), i32),
            pltpu.VMEM((2 * FC, out), bf16),
            pltpu.VMEM((1, out), f32),
            pltpu.VMEM((nb, nbr), i32),
            pltpu.VMEM((nb, nbr), i32),
            pltpu.VMEM((nb // GROUP, GROUP * slot), i32),
            pltpu.VMEM((nb // GROUP, GROUP * slot), i32),
            pltpu.VMEM((nb // GROUP, GROUP * slot), f32),
            pltpu.VMEM((2 * nb, D * R), bf16),
            pltpu.VMEM((D * R, FC), bf16),
            pltpu.VMEM((2 * nb, FC), f32),
            pltpu.VMEM((nb, 2 * FC), bf16),
            pltpu.VMEM((H, nb, share), f32),
            pltpu.VMEM((H, nb, share), f32),
            pltpu.VMEM((H - 1, nb, share), bf16),
            pltpu.VMEM((H - 1, nb, share), bf16),
            pltpu.VMEM((CHUNKS, GROUP, nb // CHUNKS), f32),
            pltpu.VMEM((CHUNKS, F - 1, GROUP, nb // CHUNKS), f32),
            dma((6,)),
            dma((Z - 1,)), dma((Z - 1,)), dma((Z * PARTS,)), dma((Z,)), dma((Z + 1,)),
            dma, dma((H * CHUNKS,)), dma, dma(((H - 1) * CHUNKS * PIECES,)), dma, dma((CHUNKS,)),
            dma((2,)), dma((2,)), flag((2,)), flag, flag,
        ],
        compiler_params=pltpu.CompilerParams(collective_id=0, has_side_effects=True),
    )(items, self_ids.reshape(1, nb), neighbor_ids.T, visit_counts.T, w_self, w_neighbor, bias.reshape(1, out))


def solution(mesh):
    placed = (
        P("dom", "feat"),
        P("dom"),
        P("dom", None),
        P("dom", None),
        P("feat", None),
        P("feat", None),
        P(),
    )
    return jax.shard_map(
        functools.partial(shards, mesh.shape["dom"], mesh.shape["feat"]),
        mesh=mesh, in_specs=placed, out_specs=P("dom", "feat"), check_vma=False,
    )
```

```python
import functools

import jax
import jax.numpy as jnp
from jax import lax
from jax.experimental import pallas as pl
from jax.experimental.pallas import tpu as pltpu
from jax.sharding import PartitionSpec as P

MESH = pl.DeviceIdType.MESH
LANES = 128
GROUP = 8
PARTS = 4
SIDE = 2
CHUNKS = 2
PIECES = 2


def kernel(
    D, F,
    items_hbm, self_hbm, ids_hbm, cnt_hbm, ws_hbm, wn_hbm, bias_hbm,
    out_ref,
    selfs, ids_t, cnt_t, w_all, bias,
    ids, cnt, key_s, lo_s, wgt_s, weights, gathered, acc, both,
    send_a, recv_a, send_b, recv_b, sq_out, sq_in,
    local_sem,
    up_send, down_send, line_recv, x_send, x_recv,
    a_send_sem, a_recv_sem, b_send_sem, b_recv_sem, q_send_sem, q_recv_sem,
    side_send, side_recv, ready_up, ready_x, ready_feat,
):
    dom, feat = lax.axis_index("dom"), lax.axis_index("feat")
    Z, H = D // 2, F // 2
    z, x = dom // 2, lax.rem(dom, 2)
    y, c = feat // 2, lax.rem(feat, 2)
    R, FC = items_hbm.shape
    nb = selfs.shape[1]
    nbr = ids.shape[1]
    share = out_ref.shape[1]
    slot = key_s.shape[1] // GROUP
    n_hi = D * R // LANES
    part = R // PARTS
    other = dom + 1 - 2 * x

    barrier = pltpu.get_barrier_semaphore()
    line = [k for k in (1, 2) if k < Z]
    lower, upper = z < Z // 2, z >= Z // 2
    inward = jnp.where(lower, 1, -1)

    def signal(sem, d, f):
        pl.semaphore_signal(sem, inc=1, device_id=(d, f), device_id_type=MESH)

    for k in line:
        pl.when(z + k < Z)(functools.partial(signal, barrier, dom + 2 * k, feat))
    pl.when(x == 0)(functools.partial(signal, barrier, other, feat))
    for k in range(1, F):
        pl.when(feat + k < F)(functools.partial(signal, barrier, dom, feat + k))

    mine = pl.ds(pl.multiple_of(dom * R, R), R)
    pairs = (
        (ids_hbm, ids_t), (cnt_hbm, cnt_t), (self_hbm, selfs), (items_hbm, gathered.at[mine, :]),
        (ws_hbm, w_all.at[0:FC]), (wn_hbm, w_all.at[FC:2 * FC]),
    )
    local = [pltpu.make_async_copy(a, b, local_sem.at[min(i, 4)]) for i, (a, b) in enumerate(pairs)]
    for copy in local[0:3]:
        copy.start()
    below = x + feat
    for k in line:
        below = below + (z >= k).astype(jnp.int32)
    pl.when(below > 0)(lambda: pl.semaphore_wait(barrier, below))

    def rows_of(block, h, n=1):
        return pl.ds(pl.multiple_of(block * R + h * part, part), n * part)

    def block_copy(block, h, n, own, send_sem, recv_sem, target):
        dst = gathered.at[rows_of(block, h, n), :]
        src = items_hbm.at[rows_of(0, h, n), :] if own else dst
        return pltpu.make_async_remote_copy(
            src_ref=src, dst_ref=dst, send_sem=send_sem, recv_sem=recv_sem,
            device_id=(target, feat), device_id_type=MESH,
        )

    def line_copy(s, h, sign, send, n=1):
        own = s < 2
        block = dom if own else dom - 2 * sign * s
        target = dom + 2 * sign * (s + 1 if own else 1)
        return block_copy(block, h, n, own, send.at[s], line_recv.at[(block // 2) * PARTS + h], target)

    def up_copy(s, h, n=1):
        return line_copy(s, h, 1, up_send, n)

    def down_copy(s, h, n=1):
        return line_copy(s, h, -1, down_send, n)

    def line_arrived(step, h):
        block = dom + 2 * step
        block_copy(block, h, 1, False, up_send.at[0], line_recv.at[(block // 2) * PARTS + h], dom).wait_recv()

    def x_copy(step, h, n=1):
        at = Z if step == 0 and h >= SIDE else z + step
        return block_copy(dom + 2 * step, h, n, step == 0, x_send.at[z + step], x_recv.at[at], other)

    def x_arrived(step, h, n):
        at = Z if h >= SIDE else z + step
        block_copy(other + 2 * step, h, n, False, x_send.at[z + step], x_recv.at[at], dom).wait_recv()

    def side_down(target):
        return block_copy(D - 1 - x, SIDE, PARTS - SIDE, False, side_send.at[0], side_recv.at[0], target)

    def side_up(target):
        return block_copy(1 - x, SIDE, PARTS - SIDE, False, side_send.at[1], side_recv.at[1], target)

    inner, outer = (z > 0) & (z < Z - 1), (z == 0) | (z == Z - 1)

    def own_down(s, low=0, high=PARTS):
        for h in range(low, high):
            down_copy(s, h).start()

    for k in reversed(line):
        pl.when(inner & (z >= k))(functools.partial(own_down, k - 1))
    @pl.when(z == Z - 1)
    def _():
        own_down(1, 0, SIDE)
        own_down(0)
        own_down(1, SIDE, PARTS)


    def across():
        for h in [*range(SIDE, PARTS), *range(SIDE)]:
            x_copy(0, h).start()

    pl.when(x == 1)(across)
    for k in line:
        pl.when(z >= k)(functools.partial(signal, ready_up.at[k - 1], dom - 2 * k, feat))
    pl.when(x == 1)(functools.partial(signal, ready_x, other, feat))
    for k in range(1, F):
        pl.when(feat >= k)(functools.partial(signal, ready_feat, dom, feat - k))
    for copy in local[3:]:
        copy.start()
    bias_load = pltpu.make_async_copy(bias_hbm, bias, local_sem.at[5])
    bias_load.start()

    def over_x(s, h, sign):
        if s == 0:
            x_copy(sign, h).start()
        else:
            end = z + s + 1 == Z - 1 if sign > 0 else z - s - 1 == 0

            @pl.when((h < SIDE) | jnp.logical_not(end))
            def _():
                x_copy(sign * (s + 1), h).start()

    def from_above(s, h):
        @pl.when(z < Z - 1 - s)
        def _():
            line_arrived(s + 1, h)
            if 0 < s < Z - 2:
                pl.when(z > 0)(lambda: down_copy(s + 1, h).start())
            over_x(s, h, 1)

    def from_below(s, h):
        @pl.when(z > s)
        def _():
            line_arrived(-(s + 1), h)
            if 0 < s < Z - 2:
                pl.when(z < Z - 1)(lambda: up_copy(s + 1, h).start())
            over_x(s, h, -1)

    def forward(s, h):
        from_above(s, h)
        from_below(s, h)

    def pass_sides():
        @pl.when((z > 0) & (z < Z - 2))
        def _():
            side_down(dom).wait_recv()
            side_down(dom - 2).start()

        @pl.when((z > 1) & (z < Z - 1))
        def _():
            side_up(dom).wait_recv()
            side_up(dom + 2).start()

    for copy in local[0:3]:
        copy.wait()
    ids[...] = jnp.transpose(ids_t[...])
    cnt[...] = jnp.transpose(cnt_t[...])
    wgt_s[...] = jnp.zeros_like(wgt_s)
    lo_s[...] = jnp.zeros_like(lo_s)
    key_s[...] = jnp.zeros_like(key_s)
    for j in range(GROUP):
        ids_j = ids[pl.ds(j, nb // GROUP, stride=GROUP), :]
        at = slice(j * slot, j * slot + nbr)
        key_s[:, at] = (ids_j // LANES) * GROUP + j
        lo_s[:, at] = lax.rem(ids_j, LANES)
        wgt_s[:, at] = cnt[pl.ds(j, nb // GROUP, stride=GROUP), :].astype(jnp.float32)

    K = key_s.shape[1]

    def half_group(g):
        key = key_s[pl.ds(g, 1), :]
        low = lo_s[pl.ds(g, 1), :]
        wgt = wgt_s[pl.ds(g, 1), :]
        left = jnp.where(lax.broadcasted_iota(jnp.int32, (n_hi * GROUP, K), 0) == key, wgt, 0.0)
        right = jnp.where(lax.broadcasted_iota(jnp.int32, (LANES, K), 0) == low, 1.0, 0.0)
        return lax.dot_general(
            left.astype(jnp.bfloat16), right.astype(jnp.bfloat16),
            (((1,), (1,)), ((), ())), preferred_element_type=jnp.float32,
        )

    def build(it, carry):
        first, second = half_group(it * 2), half_group(it * 2 + 1)
        at = pl.ds(pl.multiple_of(nb + it * 2 * GROUP, 2 * GROUP), 2 * GROUP)
        for hi in range(n_hi):
            rows = slice(hi * GROUP, (hi + 1) * GROUP)
            tile = jnp.concatenate([first[rows], second[rows]], axis=0)
            weights[at, hi * LANES:(hi + 1) * LANES] = tile.astype(jnp.bfloat16)
        return carry

    def build_pair(it, carry):
        return build(it * 2 + 1, build(it * 2, carry))

    self_col = jnp.transpose(jnp.broadcast_to(selfs[...], (LANES, nb)))
    lane = lax.broadcasted_iota(jnp.int32, (nb, LANES), 1)
    inverse = 1.0 / jnp.sum(cnt[...].astype(jnp.float32), axis=1, keepdims=True)

    @pl.when(x == 0)
    def _():
        pl.semaphore_wait(ready_x, 1)
        across()

    def own_up(k):
        pl.semaphore_wait(ready_up.at[k - 1], 1)
        for h in range(PARTS):
            up_copy(k - 1, h).start()

    for k in line:
        pl.when(z + k < Z)(functools.partial(own_up, k))

    units = nb // (4 * GROUP)
    early = units - PARTS * (-(-units // (2 * PARTS)))
    late = units - early
    lax.fori_loop(0, early, build_pair, 0)
    x_arrived(0, SIDE, PARTS - SIDE)
    pl.when(z == 0)(lambda: side_up(dom + 4).start())

    @pl.when(z == Z - 1)
    def _():
        side_down(dom - 4).start()

    def slot(h, carry):
        carry = lax.fori_loop(early + late * h // PARTS, early + late * (h + 1) // PARTS, build_pair, carry)
        pl.when(inner & (lower | (h < SIDE)))(lambda: from_below(0, h))
        pl.when(inner)(lambda: forward(1, h))
        pl.when(outer)(lambda: forward(0, h))
        return carry

    lax.fori_loop(0, PARTS, slot, 0)

    def self_weights():
        for hi in range(n_hi):
            hit = jnp.where(self_col == lane + hi * LANES, 1.0, 0.0)
            weights[0:nb, hi * LANES:(hi + 1) * LANES] = hit.astype(jnp.bfloat16)

    def add(block, low, high):
        rows = pl.ds(pl.multiple_of(block * R + low * part, part), (high - low) * part)
        at = pl.ds(pl.multiple_of(block * R + low * part, LANES), (high - low) * part)
        acc[...] += jnp.dot(weights[:, at], gathered[rows, :], preferred_element_type=jnp.float32)

    def if_there(step, work):
        pl.when((z + step >= 0) & (z + step < Z))(work)

    def add_z(step):
        def work():
            add(dom + 2 * step, 0, PARTS)
        if_there(step, work)

    def add_x(step):
        def work():
            end = z + step == (Z - 1 if step > 0 else 0)
            pl.when(end)(lambda: x_arrived(step, 0, SIDE))
            pl.when(jnp.logical_not(end))(lambda: x_arrived(step, 0, PARTS))
            pl.when(end & (z == 0))(lambda: side_down(dom).wait_recv())
            pl.when(end & (z == Z - 1))(lambda: side_up(dom).wait_recv())
            add(other + 2 * step, 0, PARTS)
        if_there(step, work)

    def add_next(step):
        def work():
            x_arrived(step, 0, PARTS)
            add(other + 2 * step, 0, PARTS)
        if_there(step, work)

    def both_ways(work, s):
        work(-s)
        work(s)

    def first_dots():
        local[3].wait()
        acc[...] = jnp.dot(weights[:, mine], gathered[mine, :], preferred_element_type=jnp.float32)
        x_arrived(0, 0, SIDE)
        add(other, 0, PARTS)

    near, far = jnp.where(outer, 1, 2), jnp.where(outer, 2, 1)
    self_weights()
    first_dots()
    both_ways(add_z, near)
    pass_sides()
    first, final = z == 0, z == Z - 1
    for h in range(PARTS):
        pl.when(inner)(functools.partial(from_above, 0, h))
        if h >= SIDE:
            pl.when(inner & upper)(functools.partial(from_below, 0, h))
    for s, h in ((1, 0), (1, 1), (2, 0), (1, 2), (2, 1), (1, 3)):
        pl.when(first & (x == 0))(functools.partial(from_above, s, h))
    for s, h in ((1, 0), (1, 1), (1, 2), (2, 0), (1, 3), (2, 1)):
        pl.when(first & (x == 1))(functools.partial(from_above, s, h))
    for s, h in ((2, 0), (1, 0), (1, 1), (2, 1), (1, 2), (1, 3)):
        pl.when(final & (x == 0))(functools.partial(from_below, s, h))
    for s, h in ((2, 0), (1, 0), (1, 1), (1, 2), (2, 1), (1, 3)):
        pl.when(final & (x == 1))(functools.partial(from_below, s, h))
    for h in range(SIDE, PARTS):
        pl.when(outer)(functools.partial(forward, 2, h))
    for s in range(2, Z - 1):
        for h in range(PARTS):
            if s < Z - 2:
                pl.when(inner)(functools.partial(forward, s, h))
            if s > 2:
                pl.when(outer)(functools.partial(forward, s, h))
    for s in range(3, Z):
        both_ways(add_z, s)
    both_ways(add_z, far)
    add_next(jnp.where(outer, inward, -inward))
    pl.when(inner)(functools.partial(both_ways, add_x, 2))
    for s in range(3, Z):
        both_ways(add_x, s)
    add_next(jnp.where(outer, 2 * inward, inward))

    pltpu.make_async_copy(w_all, w_all, local_sem.at[4]).wait()
    bias_load.wait()
    pl.when(feat < F - 1)(lambda: pl.semaphore_wait(ready_feat, F - 1 - feat))
    tall = nb // CHUNKS
    short = tall // PIECES

    def chunk(r):
        return pl.ds(r * tall, tall)

    def combine(r):
        at = slice(r * tall, (r + 1) * tall)
        both[at, 0:FC] = acc[at, :].astype(jnp.bfloat16)
        both[at, FC:2 * FC] = (acc[nb + r * tall:nb + (r + 1) * tall, :] * inverse[at]).astype(jnp.bfloat16)

    def project(r, yy, cc):
        cols = pl.ds(pl.multiple_of((yy * 2 + cc) * share, share), share)
        return jnp.dot(both[chunk(r), :], w_all[:, cols], preferred_element_type=jnp.float32)

    def a_copy(k, r):
        i = k * CHUNKS + r
        return pltpu.make_async_remote_copy(
            src_ref=send_a.at[k, chunk(r)], dst_ref=recv_a.at[k, chunk(r)],
            send_sem=a_send_sem, recv_sem=a_recv_sem.at[i],
            device_id=(dom, feat + 1 - 2 * c), device_id_type=MESH,
        )

    def b_copy(k, p):
        i = k * CHUNKS * PIECES + p
        at = pl.ds(p * short, short)
        return pltpu.make_async_remote_copy(
            src_ref=send_b.at[k, at], dst_ref=recv_b.at[k, at], send_sem=b_send_sem, recv_sem=b_recv_sem.at[i],
            device_id=(dom, lax.rem(y + k + 1, H) * 2 + c), device_id_type=MESH,
        )

    def q_copy(k, r):
        return pltpu.make_async_remote_copy(
            src_ref=sq_out.at[r], dst_ref=sq_in.at[r, k - 1], send_sem=q_send_sem, recv_sem=q_recv_sem.at[r],
            device_id=(dom, lax.rem(feat + k, F)), device_id_type=MESH,
        )

    def all_of(ref, send_sem, recv_sem):
        return pltpu.make_async_remote_copy(
            src_ref=ref, dst_ref=ref, send_sem=send_sem, recv_sem=recv_sem, device_id=(dom, feat), device_id_type=MESH,
        )

    for k in range(H):
        yy = lax.rem(y + k + 1, H)
        for r in range(CHUNKS):
            if k == 0:
                combine(r)
            send_a[k, chunk(r)] = project(r, yy, 1 - c)
            a_copy(k, r).start()
        for r in range(CHUNKS):
            here = project(r, yy, c)
            a_copy(k, r).wait_recv()
            summed = here + recv_a[k, chunk(r)]
            if k < H - 1:
                send_b[k, chunk(r)] = summed.astype(jnp.bfloat16)
                for p in range(r * PIECES, (r + 1) * PIECES):
                    b_copy(k, p).start()
            else:
                out_ref[chunk(r), :] = summed + bias[:, pl.ds(pl.multiple_of(feat * share, share), share)]

    for s in range(Z - 1):
        pl.when((z + s + 1 < Z) if s < 2 else (z < Z - 1) & (z >= s))(lambda: up_copy(s, 0, PARTS).wait_send())
        pl.when((z > s) if s < 2 else (z > 0) & (z + s < Z))(lambda: down_copy(s, 0, PARTS).wait_send())
    pl.when((z == Z - 1) | (z > 0) & (z < Z - 2))(lambda: side_down(dom - 2).wait_send())
    pl.when((z == 0) | (z > 1) & (z < Z - 1))(lambda: side_up(dom + 2).wait_send())

    def x_sent(step):
        if abs(step) < 2:
            x_copy(step, 0, PARTS).wait_send()
        else:
            end = z + step == (Z - 1 if step > 0 else 0)
            pl.when(end)(lambda: x_copy(step, 0, SIDE).wait_send())
            pl.when(jnp.logical_not(end))(lambda: x_copy(step, 0, PARTS).wait_send())

    for step in range(-(Z - 1), Z):
        if_there(step, functools.partial(x_sent, step))

    for r in range(CHUNKS):
        squares = []
        for p in range(r * PIECES, (r + 1) * PIECES):
            at = pl.ds(p * short, short)
            total = out_ref[at, :]
            for k in range(H - 1):
                b_copy(k, p).wait_recv()
                total = total + recv_b[k, at].astype(jnp.float32)
            hidden = jnp.maximum(total, 0.0)
            out_ref[at, :] = hidden
            square = hidden * hidden
            folded = square[:, 0:LANES]
            for i in range(1, share // LANES):
                folded = folded + square[:, i * LANES:(i + 1) * LANES]
            squares.append(folded)
        turned = jnp.transpose(jnp.concatenate(squares, axis=0))
        row = jnp.sum(turned, axis=0, keepdims=True)
        sq_out[r] = jnp.broadcast_to(row, (GROUP, tall))
        for k in range(1, F):
            q_copy(k, r).start()

    for r in range(CHUNKS):
        all_of(sq_in.at[r], q_send_sem, q_recv_sem.at[r]).wait_recv()
        row = sq_out[r]
        for k in range(1, F):
            row = row + sq_in[r, k - 1]
        scale = lax.rsqrt(row / (share * F) + 1e-06)[0:1, :]
        column = jnp.transpose(jnp.broadcast_to(scale, (LANES, tall)))
        for i in range(share // LANES):
            at = slice(i * LANES, (i + 1) * LANES)
            out_ref[chunk(r), at] = out_ref[chunk(r), at] * column

    all_of(send_a, a_send_sem, a_recv_sem.at[0]).wait_send()
    all_of(send_b, b_send_sem, b_recv_sem.at[0]).wait_send()
    all_of(sq_in, q_send_sem, q_recv_sem.at[0]).wait_send()


def shards(D, F, items, self_ids, neighbor_ids, visit_counts, w_self, w_neighbor, bias):
    R, FC = items.shape
    nb, nbr = neighbor_ids.shape
    out = bias.shape[0]
    share = out // F
    slot = 1 << (nbr - 1).bit_length()
    Z, H = D // 2, F // 2
    f32, bf16, i32 = jnp.float32, jnp.bfloat16, jnp.int32
    dma, flag = pltpu.SemaphoreType.DMA, pltpu.SemaphoreType.REGULAR
    return pl.pallas_call(
        functools.partial(kernel, D, F),
        out_shape=pltpu.VMEM((nb, share), f32),
        in_specs=[pl.BlockSpec(memory_space=pl.ANY)] * 7,
        out_specs=pl.BlockSpec(memory_space=pltpu.VMEM),
        scratch_shapes=[
            pltpu.VMEM((1, nb), i32),
            pltpu.VMEM((nbr, nb), i32),
            pltpu.VMEM((nbr, nb), i32),
            pltpu.VMEM((2 * FC, out), bf16),
            pltpu.VMEM((1, out), f32),
            pltpu.VMEM((nb, nbr), i32),
            pltpu.VMEM((nb, nbr), i32),
            pltpu.VMEM((nb // GROUP, GROUP * slot), i32),
            pltpu.VMEM((nb // GROUP, GROUP * slot), i32),
            pltpu.VMEM((nb // GROUP, GROUP * slot), f32),
            pltpu.VMEM((2 * nb, D * R), bf16),
            pltpu.VMEM((D * R, FC), bf16),
            pltpu.VMEM((2 * nb, FC), f32),
            pltpu.VMEM((nb, 2 * FC), bf16),
            pltpu.VMEM((H, nb, share), f32),
            pltpu.VMEM((H, nb, share), f32),
            pltpu.VMEM((H - 1, nb, share), bf16),
            pltpu.VMEM((H - 1, nb, share), bf16),
            pltpu.VMEM((CHUNKS, GROUP, nb // CHUNKS), f32),
            pltpu.VMEM((CHUNKS, F - 1, GROUP, nb // CHUNKS), f32),
            dma((6,)),
            dma((Z - 1,)), dma((Z - 1,)), dma((Z * PARTS,)), dma((Z,)), dma((Z + 1,)),
            dma, dma((H * CHUNKS,)), dma, dma(((H - 1) * CHUNKS * PIECES,)), dma, dma((CHUNKS,)),
            dma((2,)), dma((2,)), flag((2,)), flag, flag,
        ],
        compiler_params=pltpu.CompilerParams(collective_id=0, has_side_effects=True),
    )(items, self_ids.reshape(1, nb), neighbor_ids.T, visit_counts.T, w_self, w_neighbor, bias.reshape(1, out))


def solution(mesh):
    placed = (
        P("dom", "feat"),
        P("dom"),
        P("dom", None),
        P("dom", None),
        P("feat", None),
        P("feat", None),
        P(),
    )
    return jax.shard_map(
        functools.partial(shards, mesh.shape["dom"], mesh.shape["feat"]),
        mesh=mesh, in_specs=placed, out_specs=P("dom", "feat"), check_vma=False,
    )
```

```python
import functools

import jax
import jax.numpy as jnp
from jax import lax
from jax.experimental import pallas as pl
from jax.experimental.pallas import tpu as pltpu
from jax.sharding import PartitionSpec as P

MESH = pl.DeviceIdType.MESH
LANES = 128
GROUP = 8
PARTS = 4
SIDE = 2
CHUNKS = 2
PIECES = 1


def kernel(
    D, F,
    items_hbm, self_hbm, ids_hbm, cnt_hbm, ws_hbm, wn_hbm, bias_hbm,
    out_ref,
    selfs, ids_t, cnt_t, w_all, bias,
    ids, cnt, key_s, lo_s, wgt_s, weights, gathered, acc, both,
    send_a, recv_a, send_b, recv_b, sq_out, sq_in,
    local_sem,
    up_send, down_send, line_recv, x_send, x_recv,
    a_send_sem, a_recv_sem, b_send_sem, b_recv_sem, q_send_sem, q_recv_sem,
    side_send, side_recv, ready_up, ready_x, ready_feat,
):
    dom, feat = lax.axis_index("dom"), lax.axis_index("feat")
    Z, H = D // 2, F // 2
    z, x = dom // 2, lax.rem(dom, 2)
    y, c = feat // 2, lax.rem(feat, 2)
    R, FC = items_hbm.shape
    nb = selfs.shape[1]
    nbr = ids.shape[1]
    share = out_ref.shape[1]
    slot = key_s.shape[1] // GROUP
    n_hi = D * R // LANES
    part = R // PARTS
    other = dom + 1 - 2 * x

    barrier = pltpu.get_barrier_semaphore()
    line = [k for k in (1, 2) if k < Z]
    lower, upper = z < Z // 2, z >= Z // 2
    inward = jnp.where(lower, 1, -1)

    def signal(sem, d, f):
        pl.semaphore_signal(sem, inc=1, device_id=(d, f), device_id_type=MESH)

    for k in line:
        pl.when(z + k < Z)(functools.partial(signal, barrier, dom + 2 * k, feat))
    pl.when(x == 0)(functools.partial(signal, barrier, other, feat))
    for k in range(1, F):
        pl.when(feat + k < F)(functools.partial(signal, barrier, dom, feat + k))

    mine = pl.ds(pl.multiple_of(dom * R, R), R)
    pairs = (
        (ids_hbm, ids_t), (cnt_hbm, cnt_t), (self_hbm, selfs), (items_hbm, gathered.at[mine, :]),
        (ws_hbm, w_all.at[0:FC]), (wn_hbm, w_all.at[FC:2 * FC]),
    )
    local = [pltpu.make_async_copy(a, b, local_sem.at[min(i, 4)]) for i, (a, b) in enumerate(pairs)]
    for copy in local[0:3]:
        copy.start()
    below = x + feat
    for k in line:
        below = below + (z >= k).astype(jnp.int32)
    pl.when(below > 0)(lambda: pl.semaphore_wait(barrier, below))

    def rows_of(block, h, n=1):
        return pl.ds(pl.multiple_of(block * R + h * part, part), n * part)

    def block_copy(block, h, n, own, send_sem, recv_sem, target):
        dst = gathered.at[rows_of(block, h, n), :]
        src = items_hbm.at[rows_of(0, h, n), :] if own else dst
        return pltpu.make_async_remote_copy(
            src_ref=src, dst_ref=dst, send_sem=send_sem, recv_sem=recv_sem,
            device_id=(target, feat), device_id_type=MESH,
        )

    def line_copy(s, h, sign, send, n=1):
        own = s < 2
        block = dom if own else dom - 2 * sign * s
        target = dom + 2 * sign * (s + 1 if own else 1)
        return block_copy(block, h, n, own, send.at[s], line_recv.at[(block // 2) * PARTS + h], target)

    def up_copy(s, h, n=1):
        return line_copy(s, h, 1, up_send, n)

    def down_copy(s, h, n=1):
        return line_copy(s, h, -1, down_send, n)

    def line_arrived(step, h):
        block = dom + 2 * step
        block_copy(block, h, 1, False, up_send.at[0], line_recv.at[(block // 2) * PARTS + h], dom).wait_recv()

    def x_copy(step, h, n=1):
        at = Z if step == 0 and h >= SIDE else z + step
        return block_copy(dom + 2 * step, h, n, step == 0, x_send.at[z + step], x_recv.at[at], other)

    def x_arrived(step, h, n):
        at = Z if h >= SIDE else z + step
        block_copy(other + 2 * step, h, n, False, x_send.at[z + step], x_recv.at[at], dom).wait_recv()

    def side_down(target):
        return block_copy(D - 1 - x, SIDE, PARTS - SIDE, False, side_send.at[0], side_recv.at[0], target)

    def side_up(target):
        return block_copy(1 - x, SIDE, PARTS - SIDE, False, side_send.at[1], side_recv.at[1], target)

    inner, outer = (z > 0) & (z < Z - 1), (z == 0) | (z == Z - 1)

    def own_down(s, low=0, high=PARTS):
        for h in range(low, high):
            down_copy(s, h).start()

    for k in reversed(line):
        pl.when(inner & (z >= k))(functools.partial(own_down, k - 1))
    @pl.when(z == Z - 1)
    def _():
        own_down(1, 0, SIDE)
        own_down(0)
        own_down(1, SIDE, PARTS)


    def across():
        for h in [*range(SIDE, PARTS), *range(SIDE)]:
            x_copy(0, h).start()

    pl.when(x == 1)(across)
    for k in line:
        pl.when(z >= k)(functools.partial(signal, ready_up.at[k - 1], dom - 2 * k, feat))
    pl.when(x == 1)(functools.partial(signal, ready_x, other, feat))
    for k in range(1, F):
        pl.when(feat >= k)(functools.partial(signal, ready_feat, dom, feat - k))
    for copy in local[3:]:
        copy.start()
    bias_load = pltpu.make_async_copy(bias_hbm, bias, local_sem.at[5])
    bias_load.start()

    def over_x(s, h, sign):
        if s == 0:
            x_copy(sign, h).start()
        else:
            end = z + s + 1 == Z - 1 if sign > 0 else z - s - 1 == 0

            @pl.when((h < SIDE) | jnp.logical_not(end))
            def _():
                x_copy(sign * (s + 1), h).start()

    def from_above(s, h):
        @pl.when(z < Z - 1 - s)
        def _():
            line_arrived(s + 1, h)
            if 0 < s < Z - 2:
                pl.when(z > 0)(lambda: down_copy(s + 1, h).start())
            over_x(s, h, 1)

    def from_below(s, h):
        @pl.when(z > s)
        def _():
            line_arrived(-(s + 1), h)
            if 0 < s < Z - 2:
                pl.when(z < Z - 1)(lambda: up_copy(s + 1, h).start())
            over_x(s, h, -1)

    def forward(s, h):
        from_above(s, h)
        from_below(s, h)

    def pass_sides():
        @pl.when((z > 0) & (z < Z - 2))
        def _():
            side_down(dom).wait_recv()
            side_down(dom - 2).start()

        @pl.when((z > 1) & (z < Z - 1))
        def _():
            side_up(dom).wait_recv()
            side_up(dom + 2).start()

    for copy in local[0:3]:
        copy.wait()
    ids[...] = jnp.transpose(ids_t[...])
    cnt[...] = jnp.transpose(cnt_t[...])
    wgt_s[...] = jnp.zeros_like(wgt_s)
    lo_s[...] = jnp.zeros_like(lo_s)
    key_s[...] = jnp.zeros_like(key_s)
    for j in range(GROUP):
        ids_j = ids[pl.ds(j, nb // GROUP, stride=GROUP), :]
        at = slice(j * slot, j * slot + nbr)
        key_s[:, at] = (ids_j // LANES) * GROUP + j
        lo_s[:, at] = lax.rem(ids_j, LANES)
        wgt_s[:, at] = cnt[pl.ds(j, nb // GROUP, stride=GROUP), :].astype(jnp.float32)

    K = key_s.shape[1]

    def half_group(g):
        key = key_s[pl.ds(g, 1), :]
        low = lo_s[pl.ds(g, 1), :]
        wgt = wgt_s[pl.ds(g, 1), :]
        left = jnp.where(lax.broadcasted_iota(jnp.int32, (n_hi * GROUP, K), 0) == key, wgt, 0.0)
        right = jnp.where(lax.broadcasted_iota(jnp.int32, (LANES, K), 0) == low, 1.0, 0.0)
        return lax.dot_general(
            left.astype(jnp.bfloat16), right.astype(jnp.bfloat16),
            (((1,), (1,)), ((), ())), preferred_element_type=jnp.float32,
        )

    def build(it, carry):
        first, second = half_group(it * 2), half_group(it * 2 + 1)
        at = pl.ds(pl.multiple_of(nb + it * 2 * GROUP, 2 * GROUP), 2 * GROUP)
        for hi in range(n_hi):
            rows = slice(hi * GROUP, (hi + 1) * GROUP)
            tile = jnp.concatenate([first[rows], second[rows]], axis=0)
            weights[at, hi * LANES:(hi + 1) * LANES] = tile.astype(jnp.bfloat16)
        return carry

    def build_pair(it, carry):
        return build(it * 2 + 1, build(it * 2, carry))

    self_col = jnp.transpose(jnp.broadcast_to(selfs[...], (LANES, nb)))
    lane = lax.broadcasted_iota(jnp.int32, (nb, LANES), 1)
    inverse = 1.0 / jnp.sum(cnt[...].astype(jnp.float32), axis=1, keepdims=True)

    @pl.when(x == 0)
    def _():
        pl.semaphore_wait(ready_x, 1)
        across()

    def own_up(k, low=0, high=PARTS):
        if low == 0:
            pl.semaphore_wait(ready_up.at[k - 1], 1)
        for h in range(low, high):
            up_copy(k - 1, h).start()

    for k in line:
        pl.when((z > 0) & (z + k < Z))(functools.partial(own_up, k))

    @pl.when(z == 0)
    def _():
        own_up(1, 0, SIDE)
        own_up(2, 0, SIDE)
        own_up(1, SIDE, PARTS)
        own_up(2, SIDE, PARTS)


    units = nb // (4 * GROUP)
    early = units - PARTS * (-(-units // (2 * PARTS)))
    late = units - early
    lax.fori_loop(0, early, build_pair, 0)
    x_arrived(0, SIDE, PARTS - SIDE)
    pl.when(z == 0)(lambda: side_up(dom + 4).start())

    @pl.when(z == Z - 1)
    def _():
        side_down(dom - 4).start()

    def slot(h, carry):
        carry = lax.fori_loop(early + late * h // PARTS, early + late * (h + 1) // PARTS, build_pair, carry)
        pl.when(inner & (lower | (h < SIDE)))(lambda: from_below(0, h))
        pl.when(inner)(lambda: forward(1, h))
        pl.when(outer)(lambda: forward(0, h))
        return carry

    lax.fori_loop(0, PARTS, slot, 0)

    def self_weights():
        for hi in range(n_hi):
            hit = jnp.where(self_col == lane + hi * LANES, 1.0, 0.0)
            weights[0:nb, hi * LANES:(hi + 1) * LANES] = hit.astype(jnp.bfloat16)

    def add(block, low, high):
        rows = pl.ds(pl.multiple_of(block * R + low * part, part), (high - low) * part)
        at = pl.ds(pl.multiple_of(block * R + low * part, LANES), (high - low) * part)
        acc[...] += jnp.dot(weights[:, at], gathered[rows, :], preferred_element_type=jnp.float32)

    def if_there(step, work):
        pl.when((z + step >= 0) & (z + step < Z))(work)

    def add_z(step):
        def work():
            add(dom + 2 * step, 0, PARTS)
        if_there(step, work)

    def add_x(step):
        def work():
            end = z + step == (Z - 1 if step > 0 else 0)
            pl.when(end)(lambda: x_arrived(step, 0, SIDE))
            pl.when(jnp.logical_not(end))(lambda: x_arrived(step, 0, PARTS))
            pl.when(end & (z == 0))(lambda: side_down(dom).wait_recv())
            pl.when(end & (z == Z - 1))(lambda: side_up(dom).wait_recv())
            add(other + 2 * step, 0, PARTS)
        if_there(step, work)

    def add_next(step):
        def work():
            x_arrived(step, 0, PARTS)
            add(other + 2 * step, 0, PARTS)
        if_there(step, work)

    def both_ways(work, s):
        work(-s)
        work(s)

    def first_dots():
        local[3].wait()
        acc[...] = jnp.dot(weights[:, mine], gathered[mine, :], preferred_element_type=jnp.float32)
        x_arrived(0, 0, SIDE)
        add(other, 0, PARTS)

    near, far = jnp.where(outer, 1, 2), jnp.where(outer, 2, 1)
    self_weights()
    first_dots()
    both_ways(add_z, near)
    pass_sides()
    first, final = z == 0, z == Z - 1
    for h in range(PARTS):
        pl.when(inner)(functools.partial(from_above, 0, h))
        if h >= SIDE:
            pl.when(inner & upper)(functools.partial(from_below, 0, h))
    for s, h in ((1, 0), (1, 1), (2, 0), (1, 2), (2, 1), (1, 3)):
        pl.when(first & (x == 0))(functools.partial(from_above, s, h))
    for s, h in ((1, 0), (1, 1), (1, 2), (2, 0), (1, 3), (2, 1)):
        pl.when(first & (x == 1))(functools.partial(from_above, s, h))
    for s, h in ((2, 0), (1, 0), (1, 1), (2, 1), (1, 2), (1, 3)):
        pl.when(final & (x == 0))(functools.partial(from_below, s, h))
    for s, h in ((2, 0), (1, 0), (1, 1), (1, 2), (2, 1), (1, 3)):
        pl.when(final & (x == 1))(functools.partial(from_below, s, h))
    for h in range(SIDE, PARTS):
        pl.when(outer)(functools.partial(forward, 2, h))
    for s in range(2, Z - 1):
        for h in range(PARTS):
            if s < Z - 2:
                pl.when(inner)(functools.partial(forward, s, h))
            if s > 2:
                pl.when(outer)(functools.partial(forward, s, h))
    for s in range(3, Z):
        both_ways(add_z, s)
    both_ways(add_z, far)
    add_next(jnp.where(outer, inward, -inward))
    pl.when(inner)(functools.partial(both_ways, add_x, 2))
    for s in range(3, Z):
        both_ways(add_x, s)
    add_next(jnp.where(outer, 2 * inward, inward))

    pltpu.make_async_copy(w_all, w_all, local_sem.at[4]).wait()
    bias_load.wait()
    pl.when(feat < F - 1)(lambda: pl.semaphore_wait(ready_feat, F - 1 - feat))
    tall = nb // CHUNKS
    short = tall // PIECES

    def chunk(r):
        return pl.ds(r * tall, tall)

    def combine(r):
        at = slice(r * tall, (r + 1) * tall)
        both[at, 0:FC] = acc[at, :].astype(jnp.bfloat16)
        both[at, FC:2 * FC] = (acc[nb + r * tall:nb + (r + 1) * tall, :] * inverse[at]).astype(jnp.bfloat16)

    def project(r, yy, cc):
        cols = pl.ds(pl.multiple_of((yy * 2 + cc) * share, share), share)
        return jnp.dot(both[chunk(r), :], w_all[:, cols], preferred_element_type=jnp.float32)

    def a_copy(k, r):
        i = k * CHUNKS + r
        return pltpu.make_async_remote_copy(
            src_ref=send_a.at[k, chunk(r)], dst_ref=recv_a.at[k, chunk(r)],
            send_sem=a_send_sem, recv_sem=a_recv_sem.at[i],
            device_id=(dom, feat + 1 - 2 * c), device_id_type=MESH,
        )

    def b_copy(k, p):
        i = k * CHUNKS * PIECES + p
        at = pl.ds(p * short, short)
        return pltpu.make_async_remote_copy(
            src_ref=send_b.at[k, at], dst_ref=recv_b.at[k, at], send_sem=b_send_sem, recv_sem=b_recv_sem.at[i],
            device_id=(dom, lax.rem(y + k + 1, H) * 2 + c), device_id_type=MESH,
        )

    def q_copy(k, r):
        return pltpu.make_async_remote_copy(
            src_ref=sq_out.at[r], dst_ref=sq_in.at[r, k - 1], send_sem=q_send_sem, recv_sem=q_recv_sem.at[r],
            device_id=(dom, lax.rem(feat + k, F)), device_id_type=MESH,
        )

    def all_of(ref, send_sem, recv_sem):
        return pltpu.make_async_remote_copy(
            src_ref=ref, dst_ref=ref, send_sem=send_sem, recv_sem=recv_sem, device_id=(dom, feat), device_id_type=MESH,
        )

    for k in range(H):
        yy = lax.rem(y + k + 1, H)
        for r in range(CHUNKS):
            if k == 0:
                combine(r)
            send_a[k, chunk(r)] = project(r, yy, 1 - c)
            a_copy(k, r).start()
        for r in range(CHUNKS):
            here = project(r, yy, c)
            a_copy(k, r).wait_recv()
            summed = here + recv_a[k, chunk(r)]
            if k < H - 1:
                send_b[k, chunk(r)] = summed.astype(jnp.bfloat16)
                for p in range(r * PIECES, (r + 1) * PIECES):
                    b_copy(k, p).start()
            else:
                out_ref[chunk(r), :] = summed + bias[:, pl.ds(pl.multiple_of(feat * share, share), share)]

    for s in range(Z - 1):
        pl.when((z + s + 1 < Z) if s < 2 else (z < Z - 1) & (z >= s))(lambda: up_copy(s, 0, PARTS).wait_send())
        pl.when((z > s) if s < 2 else (z > 0) & (z + s < Z))(lambda: down_copy(s, 0, PARTS).wait_send())
    pl.when((z == Z - 1) | (z > 0) & (z < Z - 2))(lambda: side_down(dom - 2).wait_send())
    pl.when((z == 0) | (z > 1) & (z < Z - 1))(lambda: side_up(dom + 2).wait_send())

    def x_sent(step):
        if abs(step) < 2:
            x_copy(step, 0, PARTS).wait_send()
        else:
            end = z + step == (Z - 1 if step > 0 else 0)
            pl.when(end)(lambda: x_copy(step, 0, SIDE).wait_send())
            pl.when(jnp.logical_not(end))(lambda: x_copy(step, 0, PARTS).wait_send())

    for step in range(-(Z - 1), Z):
        if_there(step, functools.partial(x_sent, step))

    for r in range(CHUNKS):
        squares = []
        for p in range(r * PIECES, (r + 1) * PIECES):
            at = pl.ds(p * short, short)
            total = out_ref[at, :]
            for k in range(H - 1):
                b_copy(k, p).wait_recv()
                total = total + recv_b[k, at].astype(jnp.float32)
            hidden = jnp.maximum(total, 0.0)
            out_ref[at, :] = hidden
            square = hidden * hidden
            folded = square[:, 0:LANES]
            for i in range(1, share // LANES):
                folded = folded + square[:, i * LANES:(i + 1) * LANES]
            squares.append(folded)
        turned = jnp.transpose(jnp.concatenate(squares, axis=0))
        row = jnp.sum(turned, axis=0, keepdims=True)
        sq_out[r] = jnp.broadcast_to(row, (GROUP, tall))
        for k in range(1, F):
            q_copy(k, r).start()

    for r in range(CHUNKS):
        all_of(sq_in.at[r], q_send_sem, q_recv_sem.at[r]).wait_recv()
        row = sq_out[r]
        for k in range(1, F):
            row = row + sq_in[r, k - 1]
        scale = lax.rsqrt(row / (share * F) + 1e-06)[0:1, :]
        column = jnp.transpose(jnp.broadcast_to(scale, (LANES, tall)))
        for i in range(share // LANES):
            at = slice(i * LANES, (i + 1) * LANES)
            out_ref[chunk(r), at] = out_ref[chunk(r), at] * column

    all_of(send_a, a_send_sem, a_recv_sem.at[0]).wait_send()
    all_of(send_b, b_send_sem, b_recv_sem.at[0]).wait_send()
    all_of(sq_in, q_send_sem, q_recv_sem.at[0]).wait_send()


def shards(D, F, items, self_ids, neighbor_ids, visit_counts, w_self, w_neighbor, bias):
    R, FC = items.shape
    nb, nbr = neighbor_ids.shape
    out = bias.shape[0]
    share = out // F
    slot = 1 << (nbr - 1).bit_length()
    Z, H = D // 2, F // 2
    f32, bf16, i32 = jnp.float32, jnp.bfloat16, jnp.int32
    dma, flag = pltpu.SemaphoreType.DMA, pltpu.SemaphoreType.REGULAR
    return pl.pallas_call(
        functools.partial(kernel, D, F),
        out_shape=pltpu.VMEM((nb, share), f32),
        in_specs=[pl.BlockSpec(memory_space=pl.ANY)] * 7,
        out_specs=pl.BlockSpec(memory_space=pltpu.VMEM),
        scratch_shapes=[
            pltpu.VMEM((1, nb), i32),
            pltpu.VMEM((nbr, nb), i32),
            pltpu.VMEM((nbr, nb), i32),
            pltpu.VMEM((2 * FC, out), bf16),
            pltpu.VMEM((1, out), f32),
            pltpu.VMEM((nb, nbr), i32),
            pltpu.VMEM((nb, nbr), i32),
            pltpu.VMEM((nb // GROUP, GROUP * slot), i32),
            pltpu.VMEM((nb // GROUP, GROUP * slot), i32),
            pltpu.VMEM((nb // GROUP, GROUP * slot), f32),
            pltpu.VMEM((2 * nb, D * R), bf16),
            pltpu.VMEM((D * R, FC), bf16),
            pltpu.VMEM((2 * nb, FC), f32),
            pltpu.VMEM((nb, 2 * FC), bf16),
            pltpu.VMEM((H, nb, share), f32),
            pltpu.VMEM((H, nb, share), f32),
            pltpu.VMEM((H - 1, nb, share), bf16),
            pltpu.VMEM((H - 1, nb, share), bf16),
            pltpu.VMEM((CHUNKS, GROUP, nb // CHUNKS), f32),
            pltpu.VMEM((CHUNKS, F - 1, GROUP, nb // CHUNKS), f32),
            dma((6,)),
            dma((Z - 1,)), dma((Z - 1,)), dma((Z * PARTS,)), dma((Z,)), dma((Z + 1,)),
            dma, dma((H * CHUNKS,)), dma, dma(((H - 1) * CHUNKS * PIECES,)), dma, dma((CHUNKS,)),
            dma((2,)), dma((2,)), flag((2,)), flag, flag,
        ],
        compiler_params=pltpu.CompilerParams(collective_id=0, has_side_effects=True),
    )(items, self_ids.reshape(1, nb), neighbor_ids.T, visit_counts.T, w_self, w_neighbor, bias.reshape(1, out))


def solution(mesh):
    placed = (
        P("dom", "feat"),
        P("dom"),
        P("dom", None),
        P("dom", None),
        P("feat", None),
        P("feat", None),
        P(),
    )
    return jax.shard_map(
        functools.partial(shards, mesh.shape["dom"], mesh.shape["feat"]),
        mesh=mesh, in_specs=placed, out_specs=P("dom", "feat"), check_vma=False,
    )
```

```python
import functools

import jax
import jax.numpy as jnp
from jax import lax
from jax.experimental import pallas as pl
from jax.experimental.pallas import tpu as pltpu
from jax.sharding import PartitionSpec as P

MESH = pl.DeviceIdType.MESH
LANES = 128
GROUP = 8
PARTS = 4
SIDE = 2
CHUNKS = 2
PIECES = 1


def kernel(
    D, F,
    items_hbm, self_hbm, ids_hbm, cnt_hbm, ws_hbm, wn_hbm, bias_hbm,
    out_ref,
    selfs, ids_t, cnt_t, w_all, bias,
    ids, cnt, key_s, lo_s, wgt_s, weights, gathered, acc, both,
    send_a, recv_a, send_b, recv_b, sq_out, sq_in,
    local_sem,
    up_send, down_send, line_recv, x_send, x_recv,
    a_send_sem, a_recv_sem, b_send_sem, b_recv_sem, q_send_sem, q_recv_sem,
    side_send, side_recv, ready_up, ready_x, ready_feat,
):
    dom, feat = lax.axis_index("dom"), lax.axis_index("feat")
    Z, H = D // 2, F // 2
    z, x = dom // 2, lax.rem(dom, 2)
    y, c = feat // 2, lax.rem(feat, 2)
    R, FC = items_hbm.shape
    nb = selfs.shape[1]
    nbr = ids.shape[1]
    share = out_ref.shape[1]
    slot = key_s.shape[1] // GROUP
    n_hi = D * R // LANES
    part = R // PARTS
    other = dom + 1 - 2 * x

    barrier = pltpu.get_barrier_semaphore()
    line = [k for k in (1, 2) if k < Z]
    lower, upper = z < Z // 2, z >= Z // 2
    inward = jnp.where(lower, 1, -1)

    def signal(sem, d, f):
        pl.semaphore_signal(sem, inc=1, device_id=(d, f), device_id_type=MESH)

    for k in line:
        pl.when(z + k < Z)(functools.partial(signal, barrier, dom + 2 * k, feat))
    pl.when(x == 0)(functools.partial(signal, barrier, other, feat))
    for k in range(1, F):
        pl.when(feat + k < F)(functools.partial(signal, barrier, dom, feat + k))

    mine = pl.ds(pl.multiple_of(dom * R, R), R)
    pairs = (
        (ids_hbm, ids_t), (cnt_hbm, cnt_t), (self_hbm, selfs), (items_hbm, gathered.at[mine, :]),
        (ws_hbm, w_all.at[0:FC]), (wn_hbm, w_all.at[FC:2 * FC]),
    )
    local = [pltpu.make_async_copy(a, b, local_sem.at[min(i, 4)]) for i, (a, b) in enumerate(pairs)]
    for copy in local[0:3]:
        copy.start()
    below = x + feat
    for k in line:
        below = below + (z >= k).astype(jnp.int32)
    pl.when(below > 0)(lambda: pl.semaphore_wait(barrier, below))

    def rows_of(block, h, n=1):
        return pl.ds(pl.multiple_of(block * R + h * part, part), n * part)

    def block_copy(block, h, n, own, send_sem, recv_sem, target):
        dst = gathered.at[rows_of(block, h, n), :]
        src = items_hbm.at[rows_of(0, h, n), :] if own else dst
        return pltpu.make_async_remote_copy(
            src_ref=src, dst_ref=dst, send_sem=send_sem, recv_sem=recv_sem,
            device_id=(target, feat), device_id_type=MESH,
        )

    def line_copy(s, h, sign, send, n=1):
        own = s < 2
        block = dom if own else dom - 2 * sign * s
        target = dom + 2 * sign * (s + 1 if own else 1)
        return block_copy(block, h, n, own, send.at[s], line_recv.at[(block // 2) * PARTS + h], target)

    def up_copy(s, h, n=1):
        return line_copy(s, h, 1, up_send, n)

    def down_copy(s, h, n=1):
        return line_copy(s, h, -1, down_send, n)

    def line_arrived(step, h):
        block = dom + 2 * step
        block_copy(block, h, 1, False, up_send.at[0], line_recv.at[(block // 2) * PARTS + h], dom).wait_recv()

    def x_copy(step, h, n=1):
        at = Z if step == 0 and h >= SIDE else z + step
        return block_copy(dom + 2 * step, h, n, step == 0, x_send.at[z + step], x_recv.at[at], other)

    def x_arrived(step, h, n):
        at = Z if h >= SIDE else z + step
        block_copy(other + 2 * step, h, n, False, x_send.at[z + step], x_recv.at[at], dom).wait_recv()

    def side_down(target):
        return block_copy(D - 1 - x, SIDE, PARTS - SIDE, False, side_send.at[0], side_recv.at[0], target)

    def side_up(target):
        return block_copy(1 - x, SIDE, PARTS - SIDE, False, side_send.at[1], side_recv.at[1], target)

    inner, outer = (z > 0) & (z < Z - 1), (z == 0) | (z == Z - 1)

    def own_down(s, low=0, high=PARTS):
        for h in range(low, high):
            down_copy(s, h).start()

    for k in reversed(line):
        pl.when(inner & (z >= k))(functools.partial(own_down, k - 1))
    @pl.when(z == Z - 1)
    def _():
        own_down(1, 0, SIDE)
        own_down(0, 0, SIDE)
        own_down(1, SIDE, PARTS)
        own_down(0, SIDE, PARTS)


    def across():
        for h in [*range(SIDE, PARTS), *range(SIDE)]:
            x_copy(0, h).start()

    pl.when(x == 1)(across)
    for k in line:
        pl.when(z >= k)(functools.partial(signal, ready_up.at[k - 1], dom - 2 * k, feat))
    pl.when(x == 1)(functools.partial(signal, ready_x, other, feat))
    for k in range(1, F):
        pl.when(feat >= k)(functools.partial(signal, ready_feat, dom, feat - k))
    for copy in local[3:]:
        copy.start()
    bias_load = pltpu.make_async_copy(bias_hbm, bias, local_sem.at[5])
    bias_load.start()

    def over_x(s, h, sign):
        if s == 0:
            x_copy(sign, h).start()
        else:
            end = z + s + 1 == Z - 1 if sign > 0 else z - s - 1 == 0

            @pl.when((h < SIDE) | jnp.logical_not(end))
            def _():
                x_copy(sign * (s + 1), h).start()

    def from_above(s, h):
        @pl.when(z < Z - 1 - s)
        def _():
            line_arrived(s + 1, h)
            if 0 < s < Z - 2:
                pl.when(z > 0)(lambda: down_copy(s + 1, h).start())
            over_x(s, h, 1)

    def from_below(s, h):
        @pl.when(z > s)
        def _():
            line_arrived(-(s + 1), h)
            if 0 < s < Z - 2:
                pl.when(z < Z - 1)(lambda: up_copy(s + 1, h).start())
            over_x(s, h, -1)

    def forward(s, h):
        from_above(s, h)
        from_below(s, h)

    def pass_sides():
        @pl.when((z > 0) & (z < Z - 2))
        def _():
            side_down(dom).wait_recv()
            side_down(dom - 2).start()

        @pl.when((z > 1) & (z < Z - 1))
        def _():
            side_up(dom).wait_recv()
            side_up(dom + 2).start()

    for copy in local[0:3]:
        copy.wait()
    ids[...] = jnp.transpose(ids_t[...])
    cnt[...] = jnp.transpose(cnt_t[...])
    wgt_s[...] = jnp.zeros_like(wgt_s)
    lo_s[...] = jnp.zeros_like(lo_s)
    key_s[...] = jnp.zeros_like(key_s)
    for j in range(GROUP):
        ids_j = ids[pl.ds(j, nb // GROUP, stride=GROUP), :]
        at = slice(j * slot, j * slot + nbr)
        key_s[:, at] = (ids_j // LANES) * GROUP + j
        lo_s[:, at] = lax.rem(ids_j, LANES)
        wgt_s[:, at] = cnt[pl.ds(j, nb // GROUP, stride=GROUP), :].astype(jnp.float32)

    K = key_s.shape[1]

    def half_group(g):
        key = key_s[pl.ds(g, 1), :]
        low = lo_s[pl.ds(g, 1), :]
        wgt = wgt_s[pl.ds(g, 1), :]
        left = jnp.where(lax.broadcasted_iota(jnp.int32, (n_hi * GROUP, K), 0) == key, wgt, 0.0)
        right = jnp.where(lax.broadcasted_iota(jnp.int32, (LANES, K), 0) == low, 1.0, 0.0)
        return lax.dot_general(
            left.astype(jnp.bfloat16), right.astype(jnp.bfloat16),
            (((1,), (1,)), ((), ())), preferred_element_type=jnp.float32,
        )

    def build(it, carry):
        first, second = half_group(it * 2), half_group(it * 2 + 1)
        at = pl.ds(pl.multiple_of(nb + it * 2 * GROUP, 2 * GROUP), 2 * GROUP)
        for hi in range(n_hi):
            rows = slice(hi * GROUP, (hi + 1) * GROUP)
            tile = jnp.concatenate([first[rows], second[rows]], axis=0)
            weights[at, hi * LANES:(hi + 1) * LANES] = tile.astype(jnp.bfloat16)
        return carry

    def build_pair(it, carry):
        return build(it * 2 + 1, build(it * 2, carry))

    self_col = jnp.transpose(jnp.broadcast_to(selfs[...], (LANES, nb)))
    lane = lax.broadcasted_iota(jnp.int32, (nb, LANES), 1)
    inverse = 1.0 / jnp.sum(cnt[...].astype(jnp.float32), axis=1, keepdims=True)

    @pl.when(x == 0)
    def _():
        pl.semaphore_wait(ready_x, 1)
        across()

    def own_up(k, low=0, high=PARTS):
        if low == 0:
            pl.semaphore_wait(ready_up.at[k - 1], 1)
        for h in range(low, high):
            up_copy(k - 1, h).start()

    for k in line:
        pl.when((z > 0) & (z + k < Z))(functools.partial(own_up, k))

    @pl.when(z == 0)
    def _():
        own_up(1, 0, SIDE)
        own_up(2, 0, SIDE)
        own_up(1, SIDE, PARTS)
        own_up(2, SIDE, PARTS)


    units = nb // (4 * GROUP)
    early = units - PARTS * (-(-units // (2 * PARTS)))
    late = units - early
    lax.fori_loop(0, early, build_pair, 0)
    x_arrived(0, SIDE, PARTS - SIDE)
    pl.when(z == 0)(lambda: side_up(dom + 4).start())

    @pl.when(z == Z - 1)
    def _():
        side_down(dom - 4).start()

    def slot(h, carry):
        carry = lax.fori_loop(early + late * h // PARTS, early + late * (h + 1) // PARTS, build_pair, carry)
        pl.when(inner & (lower | (h < SIDE)))(lambda: from_below(0, h))
        pl.when(inner)(lambda: forward(1, h))
        pl.when(outer)(lambda: forward(0, h))
        return carry

    lax.fori_loop(0, PARTS, slot, 0)

    def self_weights():
        for hi in range(n_hi):
            hit = jnp.where(self_col == lane + hi * LANES, 1.0, 0.0)
            weights[0:nb, hi * LANES:(hi + 1) * LANES] = hit.astype(jnp.bfloat16)

    def add(block, low, high):
        rows = pl.ds(pl.multiple_of(block * R + low * part, part), (high - low) * part)
        at = pl.ds(pl.multiple_of(block * R + low * part, LANES), (high - low) * part)
        acc[...] += jnp.dot(weights[:, at], gathered[rows, :], preferred_element_type=jnp.float32)

    def if_there(step, work):
        pl.when((z + step >= 0) & (z + step < Z))(work)

    def add_z(step):
        def work():
            add(dom + 2 * step, 0, PARTS)
        if_there(step, work)

    def add_x(step):
        def work():
            end = z + step == (Z - 1 if step > 0 else 0)
            pl.when(end)(lambda: x_arrived(step, 0, SIDE))
            pl.when(jnp.logical_not(end))(lambda: x_arrived(step, 0, PARTS))
            pl.when(end & (z == 0))(lambda: side_down(dom).wait_recv())
            pl.when(end & (z == Z - 1))(lambda: side_up(dom).wait_recv())
            add(other + 2 * step, 0, PARTS)
        if_there(step, work)

    def add_next(step):
        def work():
            x_arrived(step, 0, PARTS)
            add(other + 2 * step, 0, PARTS)
        if_there(step, work)

    def both_ways(work, s):
        work(-s)
        work(s)

    def first_dots():
        local[3].wait()
        acc[...] = jnp.dot(weights[:, mine], gathered[mine, :], preferred_element_type=jnp.float32)
        x_arrived(0, 0, SIDE)
        add(other, 0, PARTS)

    near, far = jnp.where(outer, 1, 2), jnp.where(outer, 2, 1)
    self_weights()
    first_dots()
    both_ways(add_z, near)
    pass_sides()
    first, final = z == 0, z == Z - 1
    for h in range(PARTS):
        pl.when(inner)(functools.partial(from_above, 0, h))
        if h >= SIDE:
            pl.when(inner & upper)(functools.partial(from_below, 0, h))
    for s, h in ((1, 0), (1, 1), (2, 0), (1, 2), (2, 1), (1, 3)):
        pl.when(first & (x == 0))(functools.partial(from_above, s, h))
    for s, h in ((1, 0), (1, 1), (1, 2), (2, 0), (1, 3), (2, 1)):
        pl.when(first & (x == 1))(functools.partial(from_above, s, h))
    for s, h in ((2, 0), (1, 0), (1, 1), (2, 1), (1, 2), (1, 3)):
        pl.when(final & (x == 0))(functools.partial(from_below, s, h))
    for s, h in ((2, 0), (1, 0), (1, 1), (1, 2), (2, 1), (1, 3)):
        pl.when(final & (x == 1))(functools.partial(from_below, s, h))
    for h in range(SIDE, PARTS):
        pl.when(outer)(functools.partial(forward, 2, h))
    for s in range(2, Z - 1):
        for h in range(PARTS):
            if s < Z - 2:
                pl.when(inner)(functools.partial(forward, s, h))
            if s > 2:
                pl.when(outer)(functools.partial(forward, s, h))
    for s in range(3, Z):
        both_ways(add_z, s)
    both_ways(add_z, far)
    add_next(jnp.where(outer, inward, -inward))
    pl.when(inner)(functools.partial(both_ways, add_x, 2))
    for s in range(3, Z):
        both_ways(add_x, s)
    add_next(jnp.where(outer, 2 * inward, inward))

    pltpu.make_async_copy(w_all, w_all, local_sem.at[4]).wait()
    bias_load.wait()
    pl.when(feat < F - 1)(lambda: pl.semaphore_wait(ready_feat, F - 1 - feat))
    tall = nb // CHUNKS
    short = tall // PIECES

    def chunk(r):
        return pl.ds(r * tall, tall)

    def combine(r):
        at = slice(r * tall, (r + 1) * tall)
        both[at, 0:FC] = acc[at, :].astype(jnp.bfloat16)
        both[at, FC:2 * FC] = (acc[nb + r * tall:nb + (r + 1) * tall, :] * inverse[at]).astype(jnp.bfloat16)

    def project(r, yy, cc):
        cols = pl.ds(pl.multiple_of((yy * 2 + cc) * share, share), share)
        return jnp.dot(both[chunk(r), :], w_all[:, cols], preferred_element_type=jnp.float32)

    def a_copy(k, r):
        i = k * CHUNKS + r
        return pltpu.make_async_remote_copy(
            src_ref=send_a.at[k, chunk(r)], dst_ref=recv_a.at[k, chunk(r)],
            send_sem=a_send_sem, recv_sem=a_recv_sem.at[i],
            device_id=(dom, feat + 1 - 2 * c), device_id_type=MESH,
        )

    def b_copy(k, p):
        i = k * CHUNKS * PIECES + p
        at = pl.ds(p * short, short)
        return pltpu.make_async_remote_copy(
            src_ref=send_b.at[k, at], dst_ref=recv_b.at[k, at], send_sem=b_send_sem, recv_sem=b_recv_sem.at[i],
            device_id=(dom, lax.rem(y + k + 1, H) * 2 + c), device_id_type=MESH,
        )

    def q_copy(k, r):
        return pltpu.make_async_remote_copy(
            src_ref=sq_out.at[r], dst_ref=sq_in.at[r, k - 1], send_sem=q_send_sem, recv_sem=q_recv_sem.at[r],
            device_id=(dom, lax.rem(feat + k, F)), device_id_type=MESH,
        )

    def all_of(ref, send_sem, recv_sem):
        return pltpu.make_async_remote_copy(
            src_ref=ref, dst_ref=ref, send_sem=send_sem, recv_sem=recv_sem, device_id=(dom, feat), device_id_type=MESH,
        )

    for k in range(H):
        yy = lax.rem(y + k + 1, H)
        for r in range(CHUNKS):
            if k == 0:
                combine(r)
            send_a[k, chunk(r)] = project(r, yy, 1 - c)
            a_copy(k, r).start()
        for r in range(CHUNKS):
            here = project(r, yy, c)
            a_copy(k, r).wait_recv()
            summed = here + recv_a[k, chunk(r)]
            if k < H - 1:
                send_b[k, chunk(r)] = summed.astype(jnp.bfloat16)
                for p in range(r * PIECES, (r + 1) * PIECES):
                    b_copy(k, p).start()
            else:
                out_ref[chunk(r), :] = summed + bias[:, pl.ds(pl.multiple_of(feat * share, share), share)]

    for s in range(Z - 1):
        pl.when((z + s + 1 < Z) if s < 2 else (z < Z - 1) & (z >= s))(lambda: up_copy(s, 0, PARTS).wait_send())
        pl.when((z > s) if s < 2 else (z > 0) & (z + s < Z))(lambda: down_copy(s, 0, PARTS).wait_send())
    pl.when((z == Z - 1) | (z > 0) & (z < Z - 2))(lambda: side_down(dom - 2).wait_send())
    pl.when((z == 0) | (z > 1) & (z < Z - 1))(lambda: side_up(dom + 2).wait_send())

    def x_sent(step):
        if abs(step) < 2:
            x_copy(step, 0, PARTS).wait_send()
        else:
            end = z + step == (Z - 1 if step > 0 else 0)
            pl.when(end)(lambda: x_copy(step, 0, SIDE).wait_send())
            pl.when(jnp.logical_not(end))(lambda: x_copy(step, 0, PARTS).wait_send())

    for step in range(-(Z - 1), Z):
        if_there(step, functools.partial(x_sent, step))

    for r in range(CHUNKS):
        squares = []
        for p in range(r * PIECES, (r + 1) * PIECES):
            at = pl.ds(p * short, short)
            total = out_ref[at, :]
            for k in range(H - 1):
                b_copy(k, p).wait_recv()
                total = total + recv_b[k, at].astype(jnp.float32)
            hidden = jnp.maximum(total, 0.0)
            out_ref[at, :] = hidden
            square = hidden * hidden
            folded = square[:, 0:LANES]
            for i in range(1, share // LANES):
                folded = folded + square[:, i * LANES:(i + 1) * LANES]
            squares.append(folded)
        turned = jnp.transpose(jnp.concatenate(squares, axis=0))
        row = jnp.sum(turned, axis=0, keepdims=True)
        sq_out[r] = jnp.broadcast_to(row, (GROUP, tall))
        for k in range(1, F):
            q_copy(k, r).start()

    for r in range(CHUNKS):
        all_of(sq_in.at[r], q_send_sem, q_recv_sem.at[r]).wait_recv()
        row = sq_out[r]
        for k in range(1, F):
            row = row + sq_in[r, k - 1]
        scale = lax.rsqrt(row / (share * F) + 1e-06)[0:1, :]
        column = jnp.transpose(jnp.broadcast_to(scale, (LANES, tall)))
        for i in range(share // LANES):
            at = slice(i * LANES, (i + 1) * LANES)
            out_ref[chunk(r), at] = out_ref[chunk(r), at] * column

    all_of(send_a, a_send_sem, a_recv_sem.at[0]).wait_send()
    all_of(send_b, b_send_sem, b_recv_sem.at[0]).wait_send()
    all_of(sq_in, q_send_sem, q_recv_sem.at[0]).wait_send()


def shards(D, F, items, self_ids, neighbor_ids, visit_counts, w_self, w_neighbor, bias):
    R, FC = items.shape
    nb, nbr = neighbor_ids.shape
    out = bias.shape[0]
    share = out // F
    slot = 1 << (nbr - 1).bit_length()
    Z, H = D // 2, F // 2
    f32, bf16, i32 = jnp.float32, jnp.bfloat16, jnp.int32
    dma, flag = pltpu.SemaphoreType.DMA, pltpu.SemaphoreType.REGULAR
    return pl.pallas_call(
        functools.partial(kernel, D, F),
        out_shape=pltpu.VMEM((nb, share), f32),
        in_specs=[pl.BlockSpec(memory_space=pl.ANY)] * 7,
        out_specs=pl.BlockSpec(memory_space=pltpu.VMEM),
        scratch_shapes=[
            pltpu.VMEM((1, nb), i32),
            pltpu.VMEM((nbr, nb), i32),
            pltpu.VMEM((nbr, nb), i32),
            pltpu.VMEM((2 * FC, out), bf16),
            pltpu.VMEM((1, out), f32),
            pltpu.VMEM((nb, nbr), i32),
            pltpu.VMEM((nb, nbr), i32),
            pltpu.VMEM((nb // GROUP, GROUP * slot), i32),
            pltpu.VMEM((nb // GROUP, GROUP * slot), i32),
            pltpu.VMEM((nb // GROUP, GROUP * slot), f32),
            pltpu.VMEM((2 * nb, D * R), bf16),
            pltpu.VMEM((D * R, FC), bf16),
            pltpu.VMEM((2 * nb, FC), f32),
            pltpu.VMEM((nb, 2 * FC), bf16),
            pltpu.VMEM((H, nb, share), f32),
            pltpu.VMEM((H, nb, share), f32),
            pltpu.VMEM((H - 1, nb, share), bf16),
            pltpu.VMEM((H - 1, nb, share), bf16),
            pltpu.VMEM((CHUNKS, GROUP, nb // CHUNKS), f32),
            pltpu.VMEM((CHUNKS, F - 1, GROUP, nb // CHUNKS), f32),
            dma((6,)),
            dma((Z - 1,)), dma((Z - 1,)), dma((Z * PARTS,)), dma((Z,)), dma((Z + 1,)),
            dma, dma((H * CHUNKS,)), dma, dma(((H - 1) * CHUNKS * PIECES,)), dma, dma((CHUNKS,)),
            dma((2,)), dma((2,)), flag((2,)), flag, flag,
        ],
        compiler_params=pltpu.CompilerParams(collective_id=0, has_side_effects=True),
    )(items, self_ids.reshape(1, nb), neighbor_ids.T, visit_counts.T, w_self, w_neighbor, bias.reshape(1, out))


def solution(mesh):
    placed = (
        P("dom", "feat"),
        P("dom"),
        P("dom", None),
        P("dom", None),
        P("feat", None),
        P("feat", None),
        P(),
    )
    return jax.shard_map(
        functools.partial(shards, mesh.shape["dom"], mesh.shape["feat"]),
        mesh=mesh, in_specs=placed, out_specs=P("dom", "feat"), check_vma=False,
    )
```
